32 devices in a mesh: rep: 2 (over z, core), dp: 16 (over x, y).
Axes of the slice: x: 4, y: 4, z: 1, core: 2. Of those that a mesh axis runs over, the one named last changes fastest.
The devices are a block of a 4x4x8 slice.
Arguments:
- g_w_gate: bfloat16 [32, 2, 1024, 3328], P(('rep', 'dp')), parts along dimension 0
- g_w_up: bfloat16 [32, 2, 1024, 3328], P(('rep', 'dp')), parts along dimension 0
- g_w_down: bfloat16 [32, 2, 3328, 1024], P(('rep', 'dp')), parts along dimension 0
- w_gate: bfloat16 [2, 1024, 3328], replicated
- w_up: bfloat16 [2, 1024, 3328], replicated
- w_down: bfloat16 [2, 3328, 1024], replicated
- m_w_gate: float32 [2, 1024, 3328], P(None, 'dp')
- m_w_up: float32 [2, 1024, 3328], P(None, 'dp')
- m_w_down: float32 [2, 3328, 1024], P(None, 'dp')
- v_w_gate: float32 [2, 1024, 3328], P(None, 'dp')
- v_w_up: float32 [2, 1024, 3328], P(None, 'dp')
- v_w_down: float32 [2, 3328, 1024], P(None, 'dp')
Outputs:
- output 1: bfloat16 [4, 1024, 3328], P('rep'), parts along dimension 0
- output 2: bfloat16 [4, 1024, 3328], P('rep'), parts along dimension 0
- output 3: bfloat16 [4, 3328, 1024], P('rep'), parts along dimension 0
- output 4: float32 [4, 1024, 3328], P('rep', 'dp'), parts along dimension 0
- output 5: float32 [4, 1024, 3328], P('rep', 'dp'), parts along dimension 0
- output 6: float32 [4, 3328, 1024], P('rep', 'dp'), parts along dimension 0
- output 7: float32 [4, 1024, 3328], P('rep', 'dp'), parts along dimension 0
- output 8: float32 [4, 1024, 3328], P('rep', 'dp'), parts along dimension 0
- output 9: float32 [4, 3328, 1024], P('rep', 'dp'), parts along dimension 0
There are 2 independent parts. The reference program is written for one: setup_inputs(seed, part) draws one part's arguments, and reference() takes and returns one part's arrays. A program takes and returns all parts, laid end to end along the dimension named above; an argument that names none is the same for every part.
All inputs are finite; a program needn't handle non-finite values.
Results may differ from the reference program's by a relative error of at most 0.022.
Values are sent between devices in bfloat16 or wider.
A program may use at most 768 MiB of HBM per device.

```python
import jax
import jax.numpy as jnp
from jax import lax

DEVICES = 16
D = 1024
FF = 3328
LAYERS = 2
NAMES = ("w_gate", "w_up", "w_down")
SHAPES = {"w_gate": (LAYERS, D, FF), "w_up": (LAYERS, D, FF), "w_down": (LAYERS, FF, D)}


def setup_inputs(seed: int = 0, part: int = 0) -> dict:
    kz, *keys = jax.random.split(jax.random.key(seed), 1 + 5 * len(NAMES))
    loud = 2.0 ** jax.random.uniform(kz, (), jnp.float32, -1.0, 1.0)
    drawn = {}
    for name, key, both in zip(NAMES, keys[:3], keys[3:6], strict=True):
        own = jax.random.normal(jax.random.fold_in(key, part), (DEVICES, *SHAPES[name]), jnp.float32)
        shared = jax.random.normal(jax.random.fold_in(both, part), SHAPES[name], jnp.float32)
        drawn["g_" + name] = (loud * (0.7 * shared / DEVICES + 0.7 * own * DEVICES**-0.5)).astype(jnp.bfloat16)
    for name, key in zip(NAMES, keys[6:9], strict=True):
        drawn[name] = (jax.random.normal(key, SHAPES[name], jnp.float32) * SHAPES[name][1] ** -0.5).astype(jnp.bfloat16)
    for name, key in zip(NAMES, keys[9:12], strict=True):
        drawn["m_" + name] = loud * 0.5 * jax.random.normal(key, SHAPES[name], jnp.float32)
    for name, key in zip(NAMES, keys[12:15], strict=True):
        drawn["v_" + name] = loud * loud * jax.random.uniform(key, SHAPES[name], jnp.float32, 0.5, 1.5)
    return drawn


def adamw(w, m, v, g):
    m = 0.9 * m + 0.1 * g
    v = 0.95 * v + 0.05 * g * g
    step = m * lax.rsqrt(v + 1e-8) + 0.1 * w
    return (w - 0.02 * step).astype(jnp.bfloat16), m, v


def reference(g_w_gate, g_w_up, g_w_down, w_gate, w_up, w_down, m_w_gate, m_w_up, m_w_down, v_w_gate, v_w_up, v_w_down):
    def total(terms):
        return lax.scan(lambda so_far, term: (so_far + term.astype(jnp.float32), None), jnp.zeros(terms.shape[1:], jnp.float32), terms)[0]

    gradients = [total(terms).astype(jnp.bfloat16).astype(jnp.float32) for terms in (g_w_gate, g_w_up, g_w_down)]
    new = [
        adamw(w.astype(jnp.float32), m, v, g)
        for w, m, v, g in zip((w_gate, w_up, w_down), (m_w_gate, m_w_up, m_w_down), (v_w_gate, v_w_up, v_w_down), gradients, strict=True)
    ]
    return tuple(one[which] for which in range(3) for one in new)
```

```python
import math

import jax
import jax.numpy as jnp
from jax import lax
from jax.experimental import pallas as pl
from jax.experimental.pallas import tpu as pltpu
from jax.sharding import PartitionSpec as P

MESH = pl.DeviceIdType.MESH
ROWS, COLS = 16, 256
MESSAGES = 36


def adamw(w, m, v, g):
    m = 0.9 * m + 0.1 * g
    v = 0.95 * v + 0.05 * g * g
    step = m * lax.rsqrt(v + 1e-8) + 0.1 * w
    return (w - 0.02 * step).astype(jnp.bfloat16), m, v


def kernel(side, *refs):
    terms, weights, ms, vs, outs, gs = (refs[i : i + 3] for i in range(0, 18, 3))
    own, first, second = (refs[i : i + 3] for i in (18, 21, 24))
    wide, narrow = refs[27:30], refs[30:33]
    send_sem, recv_sem, load_sem, moment_sem, store_sem = (refs[i : i + 3] for i in range(33, 48, 3))

    me = lax.axis_index("dp")
    x, y = me // side, me % side
    for neighbour in ((x + 1) % side * side + y, (x + side - 1) % side * side + y, x * side + (y + 1) % side, x * side + (y + side - 1) % side):
        pl.semaphore_signal(pltpu.get_barrier_semaphore(), inc=1, device_id={"dp": neighbour}, device_id_type=MESH)
    pl.semaphore_wait(pltpu.get_barrier_semaphore(), 4)

    def place(layer):
        return x * (1 - layer) + y * layer, x * layer + y * (1 - layer)

    def index(layer, p, q):
        return (p + 2 * side) % side * (side * (1 - layer) + layer) + (q + 2 * side) % side * (1 - layer + side * layer)

    def to(layer, ring, by):
        p, q = place(layer)
        return {"dp": index(layer, p + by, q) if ring == 0 else index(layer, p, q + by)}

    def part(w, half):
        size = own[w].shape[2]
        cut = (size // ROWS + 1) // 2 * ROWS
        return (pl.ds(0, cut), pl.ds(cut, size - cut), pl.ds(0, size))[half]

    def half_of(k):
        return 2 if k < 12 or k >= 24 else (0, 1, 1, 0, 0, 1, 0, 1, 0, 1, 0, 1)[k - 12]

    def rows(w, layer, p, q, half=2):
        size = own[w].shape[2]
        inside = part(w, half)
        return pl.ds(pl.multiple_of(index(layer, p, q) * size + inside.start, ROWS), inside.size)

    def send(w, layer, k, source, target, device):
        pltpu.make_async_remote_copy(source, target, send_sem[w].at[layer, k], recv_sem[w].at[layer, k], device_id=device, device_id_type=MESH).start()

    def wait(w, layer, k, half=2):
        shape = own[w].at[layer, 0, part(w, half)]
        pltpu.make_async_copy(shape, shape, recv_sem[w].at[layer, k]).wait()

    def over_layers(f, times=1):
        def body(n, _):
            f(n % 2, n // 2) if times > 1 else f(n)
            return 0

        lax.fori_loop(0, 2 * times, body, 0)

    def blockwise(w, half, f):
        inside = part(w, half)

        def body(r, _):
            at = pl.ds(pl.multiple_of(inside.start + r * ROWS, ROWS), ROWS)
            for c in range(0, own[w].shape[3], COLS):
                f(at, pl.ds(c, COLS))
            return 0

        lax.fori_loop(0, inside.size // ROWS, body, 0)

    def add(w, layer, half, slot, *others):
        def one(at, c):
            total = own[w][layer, slot, at, c].astype(jnp.float32)
            for ref, other in others:
                total += ref[layer, other, at, c].astype(jnp.float32)
            own[w][layer, slot, at, c] = total.astype(jnp.bfloat16)

        blockwise(w, half, one)

    def load(w, layer, slot):
        p, q = place(layer)
        if isinstance(slot, int) and slot >= 4:
            at = rows(w, layer, p, q + slot - 4)
        else:
            at = rows(w, layer, p + (1 if slot < 2 else -1), q + (2, 1, 3, 0)[slot])
        return pltpu.make_async_copy(terms[w].at[0, layer, at], own[w].at[layer, slot], load_sem[w].at[layer, slot])


    def loads(w):
        def f(layer):
            for slot in range(8):
                load(w, layer, slot).start()

        over_layers(f)

    def raw1(w):
        def g(layer, j):
            p, q = place(layer)
            i = j % 2
            for k, d, by in ((0, 2 - i, 1), (2, 3 - 3 * i, -1)):
                source = terms[w].at[0, layer, rows(w, layer, p + 2, q + d)]
                send(w, layer, k + i, source, first[w].at[layer, k + i], to(layer, 0, by))

        def h(layer, i):
            p, q = place(layer)
            for k, d, by in ((4, 3 - 3 * i, 1), (6, 2 - i, -1)):
                source = terms[w].at[0, layer, rows(w, layer, p + by, q + d)]
                send(w, layer, k + i, source, first[w].at[layer, k + i], to(layer, 0, by))

        over_layers(g, 2)
        over_layers(h, 2)

    def fwd1(w):
        for i in range(2):

            def f(layer, i=i):
                for k, slot, by in ((0, 0, 1), (2, 2, -1)):
                    load(w, layer, slot + i).wait()
                    wait(w, layer, k + i)
                    add(w, layer, 2, slot + i, (first[w], k + i))
                    send(w, layer, 8 + k + i, own[w].at[layer, slot + i], first[w].at[layer, 8 + k + i], to(layer, 0, by))

            over_layers(f)

    def raw2(w):
        def f(layer):
            load(w, layer, 6).wait()
            wait(w, layer, 8)
            wait(w, layer, 6)
            add(w, layer, 2, 6, (first[w], 8), (first[w], 6))
            for half, by in ((0, 1), (1, -1)):
                at = part(w, half)
                send(w, layer, 12 + half, own[w].at[layer, 6, at], second[w].at[layer, 0, at], to(layer, 1, by))

        def g(layer):
            load(w, layer, 5).wait()
            wait(w, layer, 9)
            wait(w, layer, 7)
            add(w, layer, 1, 5, (first[w], 9), (first[w], 7))
            at = part(w, 1)
            send(w, layer, 14, own[w].at[layer, 5, at], second[w].at[layer, 1, at], to(layer, 1, 1))
            load(w, layer, 7).wait()
            wait(w, layer, 4)
            wait(w, layer, 10)
            add(w, layer, 0, 7, (first[w], 4), (first[w], 10))
            at = part(w, 0)
            send(w, layer, 15, own[w].at[layer, 7, at], second[w].at[layer, 2, at], to(layer, 1, -1))

        over_layers(f)
        over_layers(g)

    def fwd2(w):
        def f(layer):
            wait(w, layer, 12, 0)
            add(w, layer, 0, 5, (first[w], 9), (first[w], 7), (second[w], 0))
            at = part(w, 0)
            send(w, layer, 16, own[w].at[layer, 5, at], second[w].at[layer, 1, at], to(layer, 1, 1))
            wait(w, layer, 13, 1)
            add(w, layer, 1, 7, (first[w], 4), (first[w], 10), (second[w], 0))
            at = part(w, 1)
            send(w, layer, 17, own[w].at[layer, 7, at], second[w].at[layer, 2, at], to(layer, 1, -1))

        over_layers(f)

    def moments(w, layer):
        p, q = place(layer)
        slot = layer if w < 2 else 0
        return (
            pltpu.make_async_copy(ms[w].at[layer], wide[w].at[slot, 0], moment_sem[w].at[layer, 0]),
            pltpu.make_async_copy(vs[w].at[layer], wide[w].at[slot, 1], moment_sem[w].at[layer, 1]),
            pltpu.make_async_copy(weights[w].at[layer, rows(w, layer, p, q)], narrow[w].at[slot], moment_sem[w].at[layer, 2]),
        )

    def load_moments(w):
        def f(layer):
            for copy in moments(w, layer):
                copy.start()

        over_layers(f)

    def store(w, layer):
        p, q = place(layer)
        return (
            pltpu.make_async_copy(own[w].at[layer, 4], gs[w].at[layer], store_sem[w].at[layer, 0]),
            pltpu.make_async_copy(second[w].at[layer, 1], outs[w].at[layer, rows(w, layer, p, q)], store_sem[w].at[layer, 1]),
        )

    def step(w):
        def f(layer):
            p, q = place(layer)
            slot = layer if w < 2 else 0
            if w == 2:
                for copy in moments(w, layer):
                    copy.start()
            load(w, layer, 4).wait()
            for k, half in ((5, 2), (11, 2), (14, 1), (15, 0), (16, 0), (17, 1)):
                wait(w, layer, k, half)
            for copy in moments(w, layer):
                copy.wait()

            def one(at, c):
                total = own[w][layer, 4, at, c].astype(jnp.float32)
                for ref, other in ((first[w], 5), (first[w], 11), (second[w], 1), (second[w], 2)):
                    total += ref[layer, other, at, c].astype(jnp.float32)
                g = total.astype(jnp.bfloat16)
                own[w][layer, 4, at, c] = g
                old = narrow[w][slot, at, c].astype(jnp.float32)
                second[w][layer, 1, at, c] = adamw(old, wide[w][slot, 0, at, c], wide[w][slot, 1, at, c], g.astype(jnp.float32))[0]

            blockwise(w, 2, one)
            for k, half, by in ((18, 0, 1), (21, 1, -1), (19, 1, 1), (20, 0, -1)):
                source = second[w].at[layer, 1, part(w, half)]
                send(w, layer, k, source, outs[w].at[layer, rows(w, layer, p, q, half)], to(layer, 1, by))
            for copy in store(w, layer):
                copy.start()

        over_layers(f)

    def gather2(w):
        def f(layer):
            p, q = place(layer)
            for k, half, by in ((18, 0, 1), (21, 1, -1)):
                wait(w, layer, k, half)
                at = rows(w, layer, p, q - by, half)
                send(w, layer, 22 + half, outs[w].at[layer, at], outs[w].at[layer, at], to(layer, 1, by))

        over_layers(f)

    def both_ways(w, layer, d, source):
        p, q = place(layer)
        at = rows(w, layer, p, q + d)
        for k, by in ((24, 1), (28, -1)):
            send(w, layer, k + d, outs[w].at[layer, at] if source is None else source, outs[w].at[layer, at], to(layer, 0, by))

    def gather1(w):
        def f(layer):
            both_ways(w, layer, 0, second[w].at[layer, 1])
            wait(w, layer, 20, 0)
            both_ways(w, layer, 1, None)
            wait(w, layer, 19, 1)
            both_ways(w, layer, 3, None)

        over_layers(f)

    def gather1_far(w):
        def f(layer):
            wait(w, layer, 22, 0)
            wait(w, layer, 23, 1)
            both_ways(w, layer, 2, None)

        over_layers(f)

    def gather1_on(w):
        def f(layer, i):
            p, q = place(layer)
            for k, d, by in ((24, 2 * i, 1), (28, 1 + 2 * i, -1)):
                wait(w, layer, k + d)
                at = rows(w, layer, p - by, q + d)
                send(w, layer, (32 if by == 1 else 34) + i, outs[w].at[layer, at], outs[w].at[layer, at], to(layer, 0, by))

        over_layers(f, 2)

    def finish(w):
        def f(layer):
            for k in (25, 27, 28, 30, 32, 33, 34, 35):
                wait(w, layer, k)
            for k in range(MESSAGES):
                shape = own[w].at[layer, 0, part(w, half_of(k))]
                pltpu.make_async_copy(shape, shape, send_sem[w].at[layer, k]).wait()
            for copy in store(w, layer):
                copy.wait()

        over_layers(f)

    raw1(0)
    loads(0)
    load_moments(0)
    loads(1)
    fwd1(0)
    raw1(1)
    loads(2)
    raw2(0)
    fwd1(1)
    raw1(2)
    fwd2(0)
    raw2(1)
    fwd1(2)
    step(0)
    load_moments(1)
    fwd2(1)
    raw2(2)
    gather2(0)
    gather1(0)
    step(1)
    fwd2(2)
    gather1_far(0)
    gather2(1)
    gather1(1)
    step(2)
    gather1_on(0)
    gather1_far(1)
    gather2(2)
    gather1(2)
    gather1_on(1)
    gather1_far(2)
    gather1_on(2)
    for w in range(3):
        finish(w)


def solution(mesh):
    n = mesh.shape["dp"]
    side = math.isqrt(n)

    def step(*arrays):
        terms, weights, m, v = (arrays[i : i + 3] for i in (0, 3, 6, 9))
        blocks = [(one.shape[1], one.shape[2]) for one in m]
        layers = m[0].shape[0]
        anywhere = pl.BlockSpec(memory_space=pl.ANY)
        scratch = []
        for count in (8, 12, 3):
            scratch += [pltpu.VMEM((layers, count, *b), jnp.bfloat16) for b in blocks]
        kept = [2, 2, 1]
        wide = [pltpu.VMEM((k, 2, *b), jnp.float32) for k, b in zip(kept, blocks)]
        narrow = [pltpu.VMEM((k, *b), jnp.bfloat16) for k, b in zip(kept, blocks)]
        wide, narrow = [wide[0], wide[2]], [narrow[0], narrow[2]]
        for count in (MESSAGES, MESSAGES, 8, 3, 2):
            scratch += [pltpu.SemaphoreType.DMA((layers, count))] * 3

        def body(*refs):
            head, buffers, rest = refs[:27], refs[27:31], refs[31:]
            wide = (buffers[0], buffers[0], buffers[1])
            narrow = (buffers[2], buffers[2], buffers[3])
            kernel(side, *head, *wide, *narrow, *rest)

        scratch = scratch[:9] + wide + narrow + scratch[9:]
        result = pl.pallas_call(
            body,
            out_shape=[jax.ShapeDtypeStruct(w.shape, w.dtype) for w in weights] + [jax.ShapeDtypeStruct(one.shape, jnp.bfloat16) for one in m],
            in_specs=[anywhere] * 12,
            out_specs=[anywhere] * 6,
            scratch_shapes=scratch,
            compiler_params=pltpu.CompilerParams(collective_id=0, has_side_effects=True, vmem_limit_bytes=67043328),
            name="step",
        )(*arrays)
        whole, g = result[:3], result[3:]
        new = [adamw(0.0, one, two, three.astype(jnp.float32)) for one, two, three in zip(m, v, g)]
        return (*whole, *(one[1] for one in new), *(one[2] for one in new))

    all_of, cut = P(None, None, None), P(None, "dp", None)
    return jax.shard_map(
        step,
        mesh=mesh,
        in_specs=(P(("rep", "dp"), None, None, None),) * 3 + (all_of,) * 3 + (cut,) * 6,
        out_specs=(P("rep", None, None),) * 3 + (P("rep", "dp", None),) * 6,
        check_vma=False,
    )
```

```python
import math

import jax
import jax.numpy as jnp
from jax import lax
from jax.experimental import pallas as pl
from jax.experimental.pallas import tpu as pltpu
from jax.sharding import PartitionSpec as P

MESH = pl.DeviceIdType.MESH
ROWS, COLS = 16, 256
MESSAGES = 36
LIMIT = 67043328


def adamw(w, m, v, g):
    m = 0.9 * m + 0.1 * g
    v = 0.95 * v + 0.05 * g * g
    step = m * lax.rsqrt(v + 1e-8) + 0.1 * w
    return (w - 0.02 * step).astype(jnp.bfloat16), m, v


def kernel(side, *refs):
    terms, weights, ms, vs = (refs[i : i + 3] for i in range(0, 12, 3))
    outs, staged, gs = refs[12:14], refs[14:22], refs[22:25]
    own, first, second, wide, narrow = (refs[i : i + 3] for i in range(25, 40, 3))
    send_sem, recv_sem, load_sem, moment_sem, store_sem = (refs[i : i + 3] for i in range(40, 55, 3))

    me = lax.axis_index("dp")
    x, y = me // side, me % side
    for neighbour in ((x + 1) % side * side + y, (x + side - 1) % side * side + y, x * side + (y + 1) % side, x * side + (y + side - 1) % side):
        pl.semaphore_signal(pltpu.get_barrier_semaphore(), inc=1, device_id={"dp": neighbour}, device_id_type=MESH)
    pl.semaphore_wait(pltpu.get_barrier_semaphore(), 4)

    def place(layer):
        return x * (1 - layer) + y * layer, x * layer + y * (1 - layer)

    def index(layer, p, q):
        return (p + 2 * side) % side * (side * (1 - layer) + layer) + (q + 2 * side) % side * (1 - layer + side * layer)

    def to(layer, ring, by):
        p, q = place(layer)
        return {"dp": index(layer, p + by, q) if ring == 0 else index(layer, p, q + by)}

    def part(w, half):
        size = own[w].shape[2]
        cut = (size // ROWS + 1) // 2 * ROWS
        return (pl.ds(0, cut), pl.ds(cut, size - cut), pl.ds(0, size))[half]

    def half_of(k):
        return 2 if k < 12 or k >= 24 else (0, 1, 1, 0, 0, 1, 0, 1, 0, 1, 0, 1)[k - 12]

    def rows(w, layer, p, q, half=2):
        size = own[w].shape[2]
        inside = part(w, half)
        return pl.ds(pl.multiple_of(index(layer, p, q) * size + inside.start, ROWS), inside.size)

    def send(w, layer, k, source, target, device):
        pltpu.make_async_remote_copy(source, target, send_sem[w].at[layer, k], recv_sem[w].at[layer, k], device_id=device, device_id_type=MESH).start()

    def wait(w, layer, k, half=2):
        shape = own[w].at[layer, 0, part(w, half)]
        pltpu.make_async_copy(shape, shape, recv_sem[w].at[layer, k]).wait()

    def home(w, layer, d, half=2):
        p, q = place(layer)
        return staged[4 * layer + 1 - d % 2].at[d % side // 2, part(w, half)] if w == 2 else outs[w].at[layer, rows(w, layer, p, q + d, half)]

    def home_there(w, layer, d, by, half=2):
        return home(w, layer, (d - by) % side if w == 2 else d, half)

    def over_layers(f, times=1, unroll=False):
        if unroll:
            for n in range(2):
                f(n)
            return

        def body(n, _):
            f(n % 2, n // 2) if times > 1 else f(n)
            return 0

        lax.fori_loop(0, 2 * times, body, 0)

    def blockwise(w, half, f):
        inside = part(w, half)

        def body(r, _):
            at = pl.ds(pl.multiple_of(inside.start + r * ROWS, ROWS), ROWS)
            for c in range(0, own[w].shape[3], COLS):
                f(at, pl.ds(c, COLS))
            return 0

        lax.fori_loop(0, inside.size // ROWS, body, 0)

    def add(w, layer, half, slot, *others):
        def one(at, c):
            total = own[w][layer, slot, at, c].astype(jnp.float32)
            for ref, other in others:
                total += ref[layer, other, at, c].astype(jnp.float32)
            own[w][layer, slot, at, c] = total.astype(jnp.bfloat16)

        blockwise(w, half, one)

    def load(w, layer, slot):
        p, q = place(layer)
        if isinstance(slot, int) and slot >= 4:
            at = rows(w, layer, p, q + slot - 4)
        else:
            at = rows(w, layer, p + (1 if slot < 2 else -1), q + (2, 1, 3, 0)[slot])
        return pltpu.make_async_copy(terms[w].at[0, layer, at], own[w].at[layer, slot], load_sem[w].at[layer, slot])


    def loads(w):
        def f(layer):
            for slot in range(8):
                load(w, layer, slot).start()

        over_layers(f)

    def raw1(w):
        def g(layer, j):
            p, q = place(layer)
            i = j % 2
            for k, d, by in ((0, 2 - i, 1), (2, 3 - 3 * i, -1)):
                source = terms[w].at[0, layer, rows(w, layer, p + 2, q + d)]
                send(w, layer, k + i, source, first[w].at[layer, k + i], to(layer, 0, by))

        def h(layer, i):
            p, q = place(layer)
            for k, d, by in ((4, 3 - 3 * i, 1), (6, 2 - i, -1)):
                source = terms[w].at[0, layer, rows(w, layer, p + by, q + d)]
                send(w, layer, k + i, source, first[w].at[layer, k + i], to(layer, 0, by))

        over_layers(g, 2)
        over_layers(h, 2)

    def fwd1(w):
        for i in range(2):

            def f(layer, i=i):
                for k, slot, by in ((0, 0, 1), (2, 2, -1)):
                    load(w, layer, slot + i).wait()
                    wait(w, layer, k + i)
                    add(w, layer, 2, slot + i, (first[w], k + i))
                    send(w, layer, 8 + k + i, own[w].at[layer, slot + i], first[w].at[layer, 8 + k + i], to(layer, 0, by))

            over_layers(f)

    def raw2(w):
        def f(layer):
            load(w, layer, 6).wait()
            wait(w, layer, 8)
            wait(w, layer, 6)
            add(w, layer, 2, 6, (first[w], 8), (first[w], 6))
            for half, by in ((0, 1), (1, -1)):
                at = part(w, half)
                send(w, layer, 12 + half, own[w].at[layer, 6, at], second[w].at[layer, 0, at], to(layer, 1, by))

        def g(layer):
            load(w, layer, 5).wait()
            wait(w, layer, 9)
            wait(w, layer, 7)
            add(w, layer, 1, 5, (first[w], 9), (first[w], 7))
            at = part(w, 1)
            send(w, layer, 14, own[w].at[layer, 5, at], second[w].at[layer, 1, at], to(layer, 1, 1))
            load(w, layer, 7).wait()
            wait(w, layer, 4)
            wait(w, layer, 10)
            add(w, layer, 0, 7, (first[w], 4), (first[w], 10))
            at = part(w, 0)
            send(w, layer, 15, own[w].at[layer, 7, at], second[w].at[layer, 2, at], to(layer, 1, -1))

        over_layers(f)
        over_layers(g)

    def fwd2(w):
        def f(layer):
            wait(w, layer, 12, 0)
            add(w, layer, 0, 5, (first[w], 9), (first[w], 7), (second[w], 0))
            at = part(w, 0)
            send(w, layer, 16, own[w].at[layer, 5, at], second[w].at[layer, 1, at], to(layer, 1, 1))
            wait(w, layer, 13, 1)
            add(w, layer, 1, 7, (first[w], 4), (first[w], 10), (second[w], 0))
            at = part(w, 1)
            send(w, layer, 17, own[w].at[layer, 7, at], second[w].at[layer, 2, at], to(layer, 1, -1))

        over_layers(f)

    def moments(w, layer):
        p, q = place(layer)
        slot = layer if w < 2 else 0
        return (
            pltpu.make_async_copy(ms[w].at[layer], wide[w].at[slot, 0], moment_sem[w].at[layer, 0]),
            pltpu.make_async_copy(vs[w].at[layer], wide[w].at[slot, 1], moment_sem[w].at[layer, 1]),
            pltpu.make_async_copy(weights[w].at[layer, rows(w, layer, p, q)], narrow[w].at[slot], moment_sem[w].at[layer, 2]),
        )

    def load_moments(w):
        def f(layer):
            for copy in moments(w, layer):
                copy.start()

        over_layers(f)

    def store(w, layer):
        return (
            pltpu.make_async_copy(own[w].at[layer, 4], gs[w].at[layer], store_sem[w].at[layer, 0]),
            pltpu.make_async_copy(second[w].at[layer, 1], home(w, layer, 0), store_sem[w].at[layer, 1]),
        )

    def step(w):
        def f(layer):
            slot = layer if w < 2 else 0
            if w == 2:
                for copy in moments(w, layer):
                    copy.start()
            load(w, layer, 4).wait()
            for k, half in ((5, 2), (11, 2), (14, 1), (15, 0), (16, 0), (17, 1)):
                wait(w, layer, k, half)
            for copy in moments(w, layer):
                copy.wait()

            def one(at, c):
                total = own[w][layer, 4, at, c].astype(jnp.float32)
                for ref, other in ((first[w], 5), (first[w], 11), (second[w], 1), (second[w], 2)):
                    total += ref[layer, other, at, c].astype(jnp.float32)
                g = total.astype(jnp.bfloat16)
                own[w][layer, 4, at, c] = g
                old = narrow[w][slot, at, c].astype(jnp.float32)
                second[w][layer, 1, at, c] = adamw(old, wide[w][slot, 0, at, c], wide[w][slot, 1, at, c], g.astype(jnp.float32))[0]

            blockwise(w, 2, one)
            for k, half, by in ((18, 0, 1), (21, 1, -1), (19, 1, 1), (20, 0, -1)):
                source = second[w].at[layer, 1, part(w, half)]
                send(w, layer, k, source, home_there(w, layer, 0, by, half), to(layer, 1, by))
            for copy in store(w, layer):
                copy.start()

        over_layers(f, unroll=w == 2)

    def gather2(w):
        def f(layer):
            for k, half, by in ((18, 0, 1), (21, 1, -1)):
                wait(w, layer, k, half)
                send(w, layer, 22 + half, home(w, layer, -by, half), home_there(w, layer, -by, by, half), to(layer, 1, by))

        over_layers(f, unroll=w == 2)

    def both_ways(w, layer, d, source=None):
        source = home(w, layer, d) if source is None else source
        if w < 2:
            for k, by in ((24, 1), (28, -1)):
                send(w, layer, k + d, source, home(w, layer, d), to(layer, 0, by))
        else:
            k, by = (28, -1) if d % 2 else (24, 1)
            send(w, layer, k + d, source, staged[4 * layer + 2 + d % 2].at[d // 2], to(layer, 0, by))

    def gather1(w):
        def f(layer):
            both_ways(w, layer, 0, second[w].at[layer, 1])
            wait(w, layer, 20, 0)
            both_ways(w, layer, 1)
            wait(w, layer, 19, 1)
            both_ways(w, layer, 3)

        over_layers(f, unroll=w == 2)

    def gather1_far(w):
        def f(layer):
            wait(w, layer, 22, 0)
            wait(w, layer, 23, 1)
            both_ways(w, layer, 2)

        over_layers(f, unroll=w == 2)

    def gather1_on(w):
        def f(layer, i):
            p, q = place(layer)
            for k, d, by in ((24, 2 * i, 1), (28, 1 + 2 * i, -1)):
                wait(w, layer, k + d)
                at = rows(w, layer, p - by, q + d)
                send(w, layer, (32 if by == 1 else 34) + i, outs[w].at[layer, at], outs[w].at[layer, at], to(layer, 0, by))

        over_layers(f, 2)

    def finish(w):
        arrive = (24, 26, 29, 31) if w == 2 else (25, 27, 28, 30, 32, 33, 34, 35)
        leave = (*range(24), *arrive) if w == 2 else range(MESSAGES)

        def f(layer):
            for k in arrive:
                wait(w, layer, k)
            for k in leave:
                shape = own[w].at[layer, 0, part(w, half_of(k))]
                pltpu.make_async_copy(shape, shape, send_sem[w].at[layer, k]).wait()
            for copy in store(w, layer):
                copy.wait()

        over_layers(f, unroll=w == 2)

    raw1(0)
    loads(0)
    load_moments(0)
    loads(1)
    fwd1(0)
    raw1(1)
    loads(2)
    raw2(0)
    fwd1(1)
    raw1(2)
    fwd2(0)
    raw2(1)
    fwd1(2)
    step(0)
    load_moments(1)
    fwd2(1)
    raw2(2)
    gather2(0)
    gather1(0)
    step(1)
    fwd2(2)
    gather1_far(0)
    gather2(1)
    gather1(1)
    step(2)
    gather1_on(0)
    gather1_far(1)
    gather2(2)
    gather1(2)
    gather1_on(1)
    gather1_far(2)
    for w in range(3):
        finish(w)


def settle(side, *refs):
    gs, ms, vs, outs, staged = refs[:3], refs[3:6], refs[6:9], refs[9:11], refs[11:19]
    new_ms, new_vs, wholes = refs[19:22], refs[22:25], refs[25:28]
    g_at, m_at, v_at, w_at = refs[28:31], refs[31:34], refs[34:37], refs[37:40]
    moment_sem, copy_sem = refs[40:43], refs[43:46]

    copies = []
    for w in range(2):
        pieces, size = w_at[w].shape[1:3]
        for layer in range(2):
            for n in range(pieces):
                at = pl.ds(n * size, size)
                copies.append((outs[w].at[layer, at], w_at[w].at[layer, n], wholes[w].at[layer, at], copy_sem[w], (layer, n)))
    size = w_at[2].shape[2]
    for layer, number, slot, block in blocks_of(side, size, ((0, 0, (1, 3)), (1, 0, (0, 2)), (2, -1, (0, 2)), (3, 1, (1, 3)))):
        n = 2 * number + slot
        copies.append((staged[4 * layer + number].at[slot], w_at[2].at[layer, n], wholes[2].at[layer, block], copy_sem[2], (layer, n)))

    loads = [
        [[pltpu.make_async_copy(source[w].at[layer], target[w].at[layer], moment_sem[w].at[layer, n]) for n, (source, target) in enumerate(((gs, g_at), (ms, m_at), (vs, v_at)))] for layer in range(2)]
        for w in range(3)
    ]
    ins = [pltpu.make_async_copy(source, buffer, sem.at[(*at, 0)]) for source, buffer, _, sem, at in copies]
    out = [pltpu.make_async_copy(buffer, target, sem.at[(*at, 1)]) for _, buffer, target, sem, at in copies]
    for w in range(3):
        for layer in range(2):
            for copy in loads[w][layer]:
                copy.start()
    for copy in ins:
        copy.start()
    stores = []
    for w in range(3):
        for layer in range(2):
            for copy in loads[w][layer]:
                copy.wait()

            def body(r, _):
                at = pl.ds(pl.multiple_of(r * ROWS, ROWS), ROWS)
                for c in range(0, m_at[w].shape[2], COLS):
                    here = (layer, at, pl.ds(c, COLS))
                    _, m_at[w][here], v_at[w][here] = adamw(0.0, m_at[w][here], v_at[w][here], g_at[w][here].astype(jnp.float32))
                return 0

            lax.fori_loop(0, m_at[w].shape[1] // ROWS, body, 0)
            stores += [
                pltpu.make_async_copy(m_at[w].at[layer], new_ms[w].at[layer], moment_sem[w].at[layer, 3]),
                pltpu.make_async_copy(v_at[w].at[layer], new_vs[w].at[layer], moment_sem[w].at[layer, 4]),
            ]
            stores[-2].start()
            stores[-1].start()
    for one, two in zip(ins, out):
        one.wait()
        two.start()
    for copy in stores + out:
        copy.wait()


def blocks_of(side, size, arrays):
    me = lax.axis_index("dp")
    x, y = me // side, me % side
    found = []
    for layer in range(2):
        for number, dp, ds in arrays:
            for slot, d in enumerate(ds):
                first, second = (dp, d) if layer == 0 else (d, dp)
                block = (x + first + side) % side * side + (y + second + side) % side
                found.append((layer, number, slot, pl.ds(pl.multiple_of(block * size, ROWS), size)))
    return found


def patch(side, arrays, *refs):
    whole_in, brought, whole, buffer, sem = refs[0], refs[1:5], refs[5], refs[6], refs[7]
    moves = []
    for n, (layer, number, slot, block) in enumerate(blocks_of(side, buffer.shape[1], arrays)):
        moves.append(
            (
                pltpu.make_async_copy(brought[2 * layer + number].at[slot], buffer.at[n], sem.at[n, 0]),
                pltpu.make_async_copy(buffer.at[n], whole.at[layer, block], sem.at[n, 1]),
            )
        )
    for one, _ in moves:
        one.start()
    for one, two in moves:
        one.wait()
        two.start()
    for _, two in moves:
        two.wait()


def solution(mesh):
    side = math.isqrt(mesh.shape["dp"])

    def step(*arrays):
        terms, weights, m, v = (arrays[i : i + 3] for i in (0, 3, 6, 9))
        blocks = [(one.shape[1], one.shape[2]) for one in m]
        layers = m[0].shape[0]
        anywhere = pl.BlockSpec(memory_space=pl.ANY)
        scratch = []
        for count in (8, 12, 3):
            scratch += [pltpu.VMEM((layers, count, *b), jnp.bfloat16) for b in blocks]
        kept = [2, 2, 1]
        wide = [pltpu.VMEM((k, 2, *b), jnp.float32) for k, b in zip(kept, blocks)]
        narrow = [pltpu.VMEM((k, *b), jnp.bfloat16) for k, b in zip(kept, blocks)]
        wide, narrow = [wide[0], wide[2]], [narrow[0], narrow[2]]
        for count in (MESSAGES, MESSAGES, 8, 3, 2):
            scratch += [pltpu.SemaphoreType.DMA((layers, count))] * 3

        def body(*refs):
            head, buffers, rest = refs[:34], refs[34:38], refs[38:]
            wide = (buffers[0], buffers[0], buffers[1])
            narrow = (buffers[2], buffers[2], buffers[3])
            kernel(side, *head, *wide, *narrow, *rest)

        scratch = scratch[:9] + wide + narrow + scratch[9:]
        like = lambda one: jax.ShapeDtypeStruct(one.shape, one.dtype)
        block = jax.ShapeDtypeStruct((2, *blocks[2]), jnp.bfloat16)
        result = pl.pallas_call(
            body,
            out_shape=[like(w) for w in weights[:2]] + [block] * 8 + [jax.ShapeDtypeStruct(one.shape, jnp.bfloat16) for one in m],
            in_specs=[anywhere] * 12,
            out_specs=[anywhere] * 13,
            scratch_shapes=scratch,
            compiler_params=pltpu.CompilerParams(collective_id=0, has_side_effects=True, vmem_limit_bytes=LIMIT),
            name="exchange",
        )(*arrays)
        whole, staged, g = result[:2], result[2:10], result[10:]

        def on(ring, by):
            return [(x * side + y, (x + by) % side * side + y if ring == 0 else x * side + (y + by) % side) for x in range(side) for y in range(side)]

        brought = [lax.ppermute(one, "dp", on(n // 4, 1 - n % 2 * 2)) for n, one in enumerate(staged)]

        pieces = 4
        copied = [(layers, pieces, w.shape[1] // pieces, w.shape[2]) for w in weights[:2]] + [(layers, 8, *blocks[2])]
        result = pl.pallas_call(
            lambda *refs: settle(side, *refs),
            out_shape=[like(one) for one in (*m, *v, *weights)],
            in_specs=[anywhere] * 19,
            out_specs=[anywhere] * 9,
            scratch_shapes=[pltpu.VMEM((layers, *b), t) for t in (jnp.bfloat16, jnp.float32, jnp.float32) for b in blocks]
            + [pltpu.VMEM(shape, jnp.bfloat16) for shape in copied]
            + [pltpu.SemaphoreType.DMA((layers, 5))] * 3
            + [pltpu.SemaphoreType.DMA((layers, shape[1], 2)) for shape in copied],
            compiler_params=pltpu.CompilerParams(vmem_limit_bytes=LIMIT),
            cost_estimate=pl.CostEstimate(flops=6 * 3 * m[0].size, bytes_accessed=90 * 2**20, transcendentals=0),
            name="settle",
        )(*g, *m, *v, *whole, *staged)
        new_m, new_v, whole = result[:3], result[3:6], list(result[6:])

        for pair, arrays in ((0, ((0, -1, (1, 3)), (1, 1, (0, 2)))), (2, ((0, -2, (0, 2)), (1, 2, (1, 3))))):
            whole[2] = pl.pallas_call(
                lambda *refs, arrays=arrays: patch(side, arrays, *refs),
                out_shape=like(whole[2]),
                in_specs=[anywhere] * 5,
                out_specs=anywhere,
                input_output_aliases={0: 0},
                scratch_shapes=[pltpu.VMEM((8, *blocks[2]), jnp.bfloat16), pltpu.SemaphoreType.DMA((8, 2))],
                name="patch",
            )(whole[2], *(brought[4 * layer + pair + way] for layer in range(2) for way in range(2)))
        return (*whole, *new_m, *new_v)

    all_of, cut = P(None, None, None), P(None, "dp", None)
    return jax.shard_map(
        step,
        mesh=mesh,
        in_specs=(P(("rep", "dp"), None, None, None),) * 3 + (all_of,) * 3 + (cut,) * 6,
        out_specs=(P("rep", None, None),) * 3 + (P("rep", "dp", None),) * 6,
        check_vma=False,
    )
```

```python
import functools
import math

import jax
import jax.numpy as jnp
from jax import lax
from jax.experimental import pallas as pl
from jax.experimental.pallas import tpu as pltpu
from jax.sharding import PartitionSpec as P

MESH = pl.DeviceIdType.MESH
ROWS, COLS = 16, 256
LIMIT = 67043328
FAR, NEAR, FAR2, LAST, PARTS, ON, REST = 0, 2, 4, 5, 6, 9, 11
BLOCKS = (2, 2, 2, 4, 1, 4, 1, 1, 1, 2, 2, 8)


def adamw(w, m, v, g):
    m = 0.9 * m + 0.1 * g
    v = 0.95 * v + 0.05 * g * g
    step = m * lax.rsqrt(v + 1e-8) + 0.1 * w
    return (w - 0.02 * step).astype(jnp.bfloat16), m, v


def kernel(side, *refs):
    terms, weights, ms, vs = (refs[i : i + 3] for i in range(0, 12, 3))
    outs, staged, gs = refs[12:14], refs[14:18], refs[18:21]
    own, first, second, wide, narrow = (refs[i : i + 3] for i in range(21, 36, 3))
    recv_sem, (send_sem, load_sem, moment_sem, store_sem) = refs[36:39], refs[39:43]

    me = lax.axis_index("dp")
    x, y = me // side, me % side
    for neighbour in ((x + 1) % side * side + y, (x + side - 1) % side * side + y, x * side + (y + 1) % side, x * side + (y + side - 1) % side):
        pl.semaphore_signal(pltpu.get_barrier_semaphore(), inc=1, device_id={"dp": neighbour}, device_id_type=MESH)
    pl.semaphore_wait(pltpu.get_barrier_semaphore(), 4)

    def place(layer):
        return x * (1 - layer) + y * layer, x * layer + y * (1 - layer)

    def index(layer, p, q):
        return (p + 2 * side) % side * (side * (1 - layer) + layer) + (q + 2 * side) % side * (1 - layer + side * layer)

    def to(layer, ring, by):
        p, q = place(layer)
        return {"dp": index(layer, p + by, q) if ring == 0 else index(layer, p, q + by)}

    def part(w, half):
        size = own[w].shape[2]
        cut = (size // ROWS + 1) // 2 * ROWS
        return (pl.ds(0, cut), pl.ds(cut, size - cut), pl.ds(0, size))[half]

    def rows(w, layer, p, q, half=2):
        inside = part(w, half)
        return pl.ds(pl.multiple_of(index(layer, p, q) * own[w].shape[2] + inside.start, ROWS), inside.size)

    def send(w, layer, leg, group, source, target, device):
        pltpu.make_async_remote_copy(source, target, send_sem.at[w, leg], recv_sem[w].at[layer, group], device_id=device, device_id_type=MESH).start()

    def take(ref, sem):
        pltpu.make_async_copy(ref, ref, sem).wait()

    def wait(w, layer, group, blocks=None):
        take(own[w].at[layer, pl.ds(0, blocks or BLOCKS[group])] if isinstance(group, int) else own[w].at[layer, pl.ds(0, blocks)], recv_sem[w].at[layer, group])

    def home(w, layer, d, half=2):
        p, q = place(layer)
        return staged[2 * layer + 1 - d % 2].at[d % side // 2, part(w, half)] if w == 2 else outs[w].at[layer, rows(w, layer, p, q + d, half)]

    def home_there(w, layer, d, by, half=2):
        return home(w, layer, (d - by) % side if w == 2 else d, half)

    def over_layers(f, times=1, unroll=False):
        if unroll:
            for n in range(2):
                f(n)
            return

        def body(n, _):
            f(n % 2, n // 2) if times > 1 else f(n)
            return 0

        lax.fori_loop(0, 2 * times, body, 0)

    def blockwise(w, half, f):
        inside = part(w, half)

        def body(r, _):
            at = pl.ds(pl.multiple_of(inside.start + r * ROWS, ROWS), ROWS)
            for c in range(0, own[w].shape[3], COLS):
                f(at, pl.ds(c, COLS))
            return 0

        lax.fori_loop(0, inside.size // ROWS, body, 0)

    def add(w, layer, half, slot, *others):
        def one(at, c):
            total = own[w][layer, slot, at, c].astype(jnp.float32)
            for ref, other in others:
                total += ref[layer, other, at, c].astype(jnp.float32)
            own[w][layer, slot, at, c] = total.astype(jnp.bfloat16)

        blockwise(w, half, one)


    def loads(w):
        def f(layer):
            p, q = place(layer)
            for slot, (far, d) in enumerate(((1, 2), (1, 1), (-1, 3), (-1, 0), (0, 0), (0, 1), (0, 2), (0, 3))):
                pltpu.make_async_copy(terms[w].at[0, layer, rows(w, layer, p + far, q + d)], own[w].at[layer, slot], load_sem.at[w]).start()

        over_layers(f)

    def raw1(w):
        def f(layer, i):
            p, q = place(layer)
            for k, d, by in ((0, 2 - i, 1), (2, 3 - 3 * i, -1)):
                source = terms[w].at[0, layer, rows(w, layer, p + 2, q + d)]
                send(w, layer, 0, FAR + i, source, first[w].at[layer, k + i], to(layer, 0, by))

        def g(layer, i):
            p, q = place(layer)
            for k, d, by, group in ((4, 3 - 3 * i, 1, NEAR + 1 + 2 * i), (6, 2 - i, -1, NEAR + i)):
                source = terms[w].at[0, layer, rows(w, layer, p + by, q + d)]
                send(w, layer, 0, group, source, first[w].at[layer, k + i], to(layer, 0, by))

        over_layers(f, 2)
        over_layers(g, 2)

    def fwd1(w):
        take(own[w], load_sem.at[w])
        for i in range(2):

            def f(layer, i=i):
                wait(w, layer, FAR + i)
                for k, by, group in ((0, 1, NEAR + i), (2, -1, NEAR + 1 + 2 * i)):
                    add(w, layer, 2, k + i, (first[w], k + i))
                    send(w, layer, 0, group, own[w].at[layer, k + i], first[w].at[layer, 8 + k + i], to(layer, 0, by))

            over_layers(f)

    def send2(w, layer, slot, half, group, target, by):
        at = part(w, half)
        send(w, layer, 1, group, own[w].at[layer, slot, at], second[w].at[layer, target, at], to(layer, 1, by))

    def raw2(w):
        def f(layer):
            wait(w, layer, NEAR)
            add(w, layer, 2, 6, (first[w], 8), (first[w], 6))
            send2(w, layer, 6, 0, FAR2, 0, 1)
            send2(w, layer, 6, 1, FAR2, 0, -1)

        def g(layer):
            wait(w, layer, NEAR + 1)
            add(w, layer, 1, 5, (first[w], 9), (first[w], 7))
            send2(w, layer, 5, 1, LAST, 1, 1)
            add(w, layer, 0, 7, (first[w], 4), (first[w], 10))
            send2(w, layer, 7, 0, LAST, 2, -1)

        over_layers(f)
        over_layers(g)

    def fwd2(w):
        def f(layer):
            wait(w, layer, FAR2)
            add(w, layer, 0, 5, (first[w], 9), (first[w], 7), (second[w], 0))
            send2(w, layer, 5, 0, LAST, 1, 1)
            add(w, layer, 1, 7, (first[w], 4), (first[w], 10), (second[w], 0))
            send2(w, layer, 7, 1, LAST, 2, -1)

        over_layers(f)

    def load_moments(w, layer):
        p, q = place(layer)
        slot = layer if w < 2 else 0
        pltpu.make_async_copy(ms[w].at[layer], wide[w].at[slot, 0], moment_sem.at[w, 0]).start()
        pltpu.make_async_copy(vs[w].at[layer], wide[w].at[slot, 1], moment_sem.at[w, 0]).start()
        pltpu.make_async_copy(weights[w].at[layer, rows(w, layer, p, q)], narrow[w].at[slot], moment_sem.at[w, 1]).start()

    def take_moments(w):
        take(wide[w], moment_sem.at[w, 0])
        take(narrow[w], moment_sem.at[w, 1])

    def step(w):
        if w < 2:
            take_moments(w)

        def f(layer):
            slot = layer if w < 2 else 0
            if w == 2:
                load_moments(w, layer)
            wait(w, layer, LAST)
            if w == 2:
                take_moments(w)

            def one(at, c):
                total = own[w][layer, 4, at, c].astype(jnp.float32)
                for ref, other in ((first[w], 5), (first[w], 11), (second[w], 1), (second[w], 2)):
                    total += ref[layer, other, at, c].astype(jnp.float32)
                g = total.astype(jnp.bfloat16)
                own[w][layer, 4, at, c] = g
                old = narrow[w][slot, at, c].astype(jnp.float32)
                second[w][layer, 1, at, c] = adamw(old, wide[w][slot, 0, at, c], wide[w][slot, 1, at, c], g.astype(jnp.float32))[0]

            blockwise(w, 2, one)
            for group, half, by in ((PARTS, 1, 1), (PARTS, 0, -1), (PARTS + 1, 0, 1), (PARTS + 1, 1, -1)):
                source = second[w].at[layer, 1, part(w, half)]
                send(w, layer, 2, group, source, home_there(w, layer, 0, by, half), to(layer, 1, by))
            pltpu.make_async_copy(own[w].at[layer, 4], gs[w].at[layer], store_sem.at[w, 0]).start()
            pltpu.make_async_copy(second[w].at[layer, 1], home(w, layer, 0), store_sem.at[w, 1]).start()

        over_layers(f, unroll=w == 2)

    def gather2(w):
        def f(layer):
            wait(w, layer, PARTS)
            for half, by in ((1, 1), (0, -1)):
                send(w, layer, 2, PARTS + 2, home(w, layer, -by, half), home_there(w, layer, -by, by, half), to(layer, 1, by))

        over_layers(f, unroll=w == 2)

    def give(w, layer, d, source=None):
        source = home(w, layer, d) if source is None else source
        for by in (1, -1):
            on = (by == 1) == (d % 2 == 0)
            if w < 2:
                send(w, layer, 3, ON + d // 2 if on else REST, source, home(w, layer, d), to(layer, 0, by))
            elif on:
                send(w, layer, 3, REST, source, staged[2 * layer + d % 2].at[2 + d // 2], to(layer, 0, by))

    def gather1(w):
        def f(layer):
            give(w, layer, 0, second[w].at[layer, 1])
            wait(w, layer, PARTS + 1)
            give(w, layer, 1)
            give(w, layer, 3)

        over_layers(f, unroll=w == 2)

    def gather1_far(w):
        def f(layer):
            wait(w, layer, PARTS + 2)
            give(w, layer, 2)

        over_layers(f, unroll=w == 2)

    def gather1_on(w):
        def f(layer, i):
            p, q = place(layer)
            wait(w, layer, ON + i, 2)
            for d, by in ((2 * i, 1), (1 + 2 * i, -1)):
                at = outs[w].at[layer, rows(w, layer, p - by, q + d)]
                send(w, layer, 3, REST, at, at, to(layer, 0, by))

        over_layers(f, 2)

    def finish(w):
        for layer in range(2):
            wait(w, layer, REST, 4 if w == 2 else 8)
        for leg, ref in enumerate((first[w], second[w], second[w], own[w].at[0] if w == 2 else first[w])):
            take(ref, send_sem.at[w, leg])
        for n in range(2):
            take(gs[w], store_sem.at[w, n])

    raw1(0)
    loads(0)
    over_layers(lambda layer: load_moments(0, layer))
    loads(1)
    fwd1(0)
    raw1(1)
    loads(2)
    raw2(0)
    fwd1(1)
    raw1(2)
    fwd2(0)
    raw2(1)
    fwd1(2)
    step(0)
    over_layers(lambda layer: load_moments(1, layer))
    fwd2(1)
    raw2(2)
    gather2(0)
    gather1(0)
    step(1)
    fwd2(2)
    gather1_far(0)
    gather2(1)
    gather1(1)
    step(2)
    gather1_on(0)
    gather1_far(1)
    gather2(2)
    gather1(2)
    gather1_on(1)
    gather1_far(2)
    for w in range(3):
        finish(w)


def spots(side, size, shift):
    me = lax.axis_index("dp")
    for layer in range(2):
        for way in range(2):
            for slot in range(side):
                far = (2 * way - 1) * (shift + slot // 2)
                d = (1 - way + slot // 2) % 2 + 2 * (slot % 2)
                a, b = (far, d) if layer == 0 else (d, far)
                block = (me // side + a + side) % side * side + (me % side + b + side) % side
                yield layer, way, slot, pl.ds(pl.multiple_of(block * size, ROWS), size)


def settle(side, *refs):
    gs, ms, vs, outs, staged = refs[:3], refs[3:6], refs[6:9], refs[9:11], refs[11:15]
    new_ms, new_vs, wholes = refs[15:18], refs[18:21], refs[21:24]
    g_at, m_at, v_at, w_at = refs[24:27], refs[27:30], refs[30:33], refs[33:36]
    moment_sem, store_sem, *copy_sem = refs[36:41]

    copies = []
    for w in range(2):
        pieces, size = w_at[w].shape[1:3]
        for layer in range(2):
            for n in range(pieces):
                at = pl.ds(n * size, size)
                copies.append((outs[w].at[layer, at], w_at[w].at[layer, n], wholes[w].at[layer, at], copy_sem[w].at[layer, n]))
    for layer, way, slot, at in spots(side, w_at[2].shape[2], 0):
        n = way * side + slot
        copies.append((staged[2 * layer + way].at[slot], w_at[2].at[layer, n], wholes[2].at[layer, at], copy_sem[2].at[layer, n]))

    for w in range(3):
        for n, (source, target) in enumerate(((gs, g_at), (ms, m_at), (vs, v_at))):
            pltpu.make_async_copy(source[w], target[w], moment_sem.at[w, n]).start()
    for source, buffer, _, sem in copies:
        pltpu.make_async_copy(source, buffer, sem).start()
    stores = []
    for w in range(3):
        for n, (source, target) in enumerate(((gs, g_at), (ms, m_at), (vs, v_at))):
            pltpu.make_async_copy(source[w], target[w], moment_sem.at[w, n]).wait()

        def body(r, _, w=w):
            for layer in range(2):
                at = pl.ds(pl.multiple_of(r * ROWS, ROWS), ROWS)
                for c in range(0, m_at[w].shape[2], COLS):
                    here = (layer, at, pl.ds(c, COLS))
                    _, m_at[w][here], v_at[w][here] = adamw(0.0, m_at[w][here], v_at[w][here], g_at[w][here].astype(jnp.float32))
            return 0

        lax.fori_loop(0, m_at[w].shape[1] // ROWS, body, 0)
        stores += [pltpu.make_async_copy(a[w], b[w], store_sem.at[w, n]) for n, (a, b) in enumerate(((m_at, new_ms), (v_at, new_vs)))]
        stores[-2].start()
        stores[-1].start()
    for source, buffer, target, sem in copies:
        pltpu.make_async_copy(source, buffer, sem).wait()
        stores.append(pltpu.make_async_copy(buffer, target, sem))
        stores[-1].start()
    for copy in stores:
        copy.wait()


def patch(side, *refs):
    brought, whole, buffer, sem = refs[1:5], refs[5], refs[6], refs[7]
    moves = []
    for n, (layer, way, slot, at) in enumerate(spots(side, buffer.shape[1], 1)):
        ends = (brought[2 * layer + way].at[slot], buffer.at[n], whole.at[layer, at])
        moves.append([pltpu.make_async_copy(*pair, sem.at[n]) for pair in zip(ends, ends[1:])])
    for one, _ in moves:
        one.start()
    for one, two in moves:
        one.wait()
        two.start()
    for _, two in moves:
        two.wait()


def solution(mesh):
    side = math.isqrt(mesh.shape["dp"])

    def on(ring, by):
        return [(x * side + y, (x + by) % side * side + y if ring == 0 else x * side + (y + by) % side) for x in range(side) for y in range(side)]

    def step(*arrays):
        weights, m, v = (arrays[i : i + 3] for i in (3, 6, 9))
        blocks = [one.shape[1:] for one in m]
        layers = m[0].shape[0]
        bf16, f32, dma = jnp.bfloat16, jnp.float32, pltpu.SemaphoreType.DMA
        anywhere = pl.BlockSpec(memory_space=pl.ANY)

        def call(f, name, inputs, outputs, scratch, params, **more):
            return pl.pallas_call(
                f,
                out_shape=[jax.ShapeDtypeStruct(one.shape, one.dtype) for one in outputs],
                in_specs=[anywhere] * len(inputs),
                out_specs=[anywhere] * len(outputs),
                scratch_shapes=scratch,
                compiler_params=pltpu.CompilerParams(vmem_limit_bytes=LIMIT, **params),
                name=name,
                **more,
            )(*inputs)

        scratch = [pltpu.VMEM((layers, count, *b), bf16) for count in (8, 12, 3) for b in blocks]
        scratch += [pltpu.VMEM((k, 2, *blocks[w]), f32) for w, k in ((0, layers), (2, 1))]
        scratch += [pltpu.VMEM((k, *blocks[w]), bf16) for w, k in ((0, layers), (2, 1))]
        scratch += [dma((layers, len(BLOCKS)))] * 3 + [dma((3, 4)), dma((3,)), dma((3, 2)), dma((3, 2))]

        def exchange(*refs):
            head, (wide, wide2, narrow, narrow2), sems = refs[:30], refs[30:34], refs[34:]
            kernel(side, *head, wide, wide, wide2, narrow, narrow, narrow2, *sems)

        stage = jax.ShapeDtypeStruct((side, *blocks[2]), bf16)
        g = [jax.ShapeDtypeStruct(one.shape, bf16) for one in m]
        result = call(exchange, "exchange", arrays, [*weights[:2], *[stage] * 4, *g], scratch, {"collective_id": 0, "has_side_effects": True})
        whole, staged, g = result[:2], result[2:6], result[6:]
        brought = [lax.ppermute(one, "dp", on(n // 2, 1 - n % 2 * 2)) for n, one in enumerate(staged)]

        copied = [(layers, side, w.shape[1] // side, w.shape[2]) for w in weights[:2]] + [(layers, 2 * side, *blocks[2])]
        scratch = [pltpu.VMEM(one.shape, t) for t in (bf16, f32, f32) for one in m] + [pltpu.VMEM(shape, bf16) for shape in copied]
        scratch += [dma((3, 3)), dma((3, 2))] + [dma(shape[:2]) for shape in copied]
        cost = pl.CostEstimate(flops=18 * m[0].size, bytes_accessed=5 * weights[0].size, transcendentals=0)
        result = call(functools.partial(settle, side), "settle", [*g, *m, *v, *whole, *staged], [*m, *v, *weights], scratch, {}, cost_estimate=cost)
        *moments, gate, up, down = result
        scratch = [pltpu.VMEM((4 * side, *blocks[2]), bf16), dma((4 * side,))]
        (down,) = call(functools.partial(patch, side), "patch", [down, *brought], [down], scratch, {}, input_output_aliases={0: 0})
        return (gate, up, down, *moments)

    all_of, cut = P(None, None, None), P(None, "dp", None)
    return jax.shard_map(
        step,
        mesh=mesh,
        in_specs=(P(("rep", "dp"), None, None, None),) * 3 + (all_of,) * 3 + (cut,) * 6,
        out_specs=(P("rep", None, None),) * 3 + (P("rep", "dp", None),) * 6,
        check_vma=False,
    )
```

```python
import functools
import math

import jax
import jax.numpy as jnp
from jax import lax
from jax.experimental import pallas as pl
from jax.experimental.pallas import tpu as pltpu
from jax.sharding import PartitionSpec as P

MESH = pl.DeviceIdType.MESH
ROWS, COLS = 16, 256
LIMIT = 67043328
FAR, NEAR, FAR2, LAST, PARTS, ON, REST = 0, 2, 4, 5, 6, 9, 11
BLOCKS = (2, 2, 2, 4, 1, 4, 1, 1, 1, 2, 2, 8)


def adamw(w, m, v, g):
    m = 0.9 * m + 0.1 * g
    v = 0.95 * v + 0.05 * g * g
    step = m * lax.rsqrt(v + 1e-8) + 0.1 * w
    return (w - 0.02 * step).astype(jnp.bfloat16), m, v


def kernel(side, *refs):
    terms, weights, ms, vs = (refs[i : i + 3] for i in range(0, 12, 3))
    outs, staged, gs = refs[12:14], refs[14:18], refs[18:21]
    own, first, second, wide, narrow = (refs[i : i + 3] for i in range(21, 36, 3))
    recv_sem, (send_sem, load_sem, moment_sem, store_sem) = refs[36:39], refs[39:43]

    me = lax.axis_index("dp")
    x, y = me // side, me % side
    for neighbour in ((x + 1) % side * side + y, (x + side - 1) % side * side + y, x * side + (y + 1) % side, x * side + (y + side - 1) % side):
        pl.semaphore_signal(pltpu.get_barrier_semaphore(), inc=1, device_id={"dp": neighbour}, device_id_type=MESH)
    pl.semaphore_wait(pltpu.get_barrier_semaphore(), 4)

    def place(layer):
        return x * (1 - layer) + y * layer, x * layer + y * (1 - layer)

    def index(layer, p, q):
        return (p + 2 * side) % side * (side * (1 - layer) + layer) + (q + 2 * side) % side * (1 - layer + side * layer)

    def to(layer, ring, by):
        p, q = place(layer)
        return {"dp": index(layer, p + by, q) if ring == 0 else index(layer, p, q + by)}

    def part(w, half):
        size = own[w].shape[2]
        cut = (size // ROWS + 1) // 2 * ROWS
        return (pl.ds(0, cut), pl.ds(cut, size - cut), pl.ds(0, size))[half]

    def rows(w, layer, p, q, half=2):
        inside = part(w, half)
        return pl.ds(pl.multiple_of(index(layer, p, q) * own[w].shape[2] + inside.start, ROWS), inside.size)

    def send(w, layer, leg, group, source, target, device):
        pltpu.make_async_remote_copy(source, target, send_sem.at[w, leg], recv_sem[w].at[layer, group], device_id=device, device_id_type=MESH).start()

    def take(ref, sem):
        pltpu.make_async_copy(ref, ref, sem).wait()

    def wait(w, layer, group, blocks=None):
        take(own[w].at[layer, pl.ds(0, blocks or BLOCKS[group])] if isinstance(group, int) else own[w].at[layer, pl.ds(0, blocks)], recv_sem[w].at[layer, group])

    def home(w, layer, d, half=2):
        p, q = place(layer)
        return staged[2 * layer + 1 - d % 2].at[d % side // 2, part(w, half)] if w == 2 else outs[w].at[layer, rows(w, layer, p, q + d, half)]

    def home_there(w, layer, d, by, half=2):
        return home(w, layer, (d - by) % side if w == 2 else d, half)

    def over_layers(f, times=1, unroll=False):
        if unroll:
            for n in range(2):
                f(n)
            return

        def body(n, _):
            f(n % 2, n // 2) if times > 1 else f(n)
            return 0

        lax.fori_loop(0, 2 * times, body, 0)

    def blockwise(w, half, f):
        inside = part(w, half)

        def body(r, _):
            at = pl.ds(pl.multiple_of(inside.start + r * ROWS, ROWS), ROWS)
            for c in range(0, own[w].shape[3], COLS):
                f(at, pl.ds(c, COLS))
            return 0

        lax.fori_loop(0, inside.size // ROWS, body, 0)

    def add(w, layer, half, slot, *others):
        def one(at, c):
            total = own[w][layer, slot, at, c].astype(jnp.float32)
            for ref, other in others:
                total += ref[layer, other, at, c].astype(jnp.float32)
            own[w][layer, slot, at, c] = total.astype(jnp.bfloat16)

        blockwise(w, half, one)


    def loads(w):
        def f(layer):
            p, q = place(layer)
            for slot, (far, d) in enumerate(((1, 2), (1, 1), (-1, 3), (-1, 0), (0, 0), (0, 1), (0, 2), (0, 3))):
                pltpu.make_async_copy(terms[w].at[0, layer, rows(w, layer, p + far, q + d)], own[w].at[layer, slot], load_sem.at[w]).start()

        over_layers(f)

    def raw1(w):
        def f(layer, i):
            p, q = place(layer)
            for k, d, by in ((0, 2 - i, 1), (2, 3 - 3 * i, -1)):
                source = terms[w].at[0, layer, rows(w, layer, p + 2, q + d)]
                send(w, layer, 0, FAR + i, source, first[w].at[layer, k + i], to(layer, 0, by))

        def g(layer, i):
            p, q = place(layer)
            for k, d, by, group in ((4, 3 - 3 * i, 1, NEAR + 1 + 2 * i), (6, 2 - i, -1, NEAR + i)):
                source = terms[w].at[0, layer, rows(w, layer, p + by, q + d)]
                send(w, layer, 0, group, source, first[w].at[layer, k + i], to(layer, 0, by))

        over_layers(f, 2)
        over_layers(g, 2)

    def fwd1(w):
        take(own[w], load_sem.at[w])
        for i in range(2):

            def f(layer, i=i):
                wait(w, layer, FAR + i)
                for k, by, group in ((0, 1, NEAR + i), (2, -1, NEAR + 1 + 2 * i)):
                    add(w, layer, 2, k + i, (first[w], k + i))
                    send(w, layer, 0, group, own[w].at[layer, k + i], first[w].at[layer, 8 + k + i], to(layer, 0, by))

            over_layers(f)

    def send2(w, layer, slot, half, group, target, by):
        at = part(w, half)
        send(w, layer, 1, group, own[w].at[layer, slot, at], second[w].at[layer, target, at], to(layer, 1, by))

    def raw2(w):
        def f(layer):
            wait(w, layer, NEAR)
            add(w, layer, 2, 6, (first[w], 8), (first[w], 6))
            send2(w, layer, 6, 0, FAR2, 0, 1)
            send2(w, layer, 6, 1, FAR2, 0, -1)

        def g(layer):
            wait(w, layer, NEAR + 1)
            add(w, layer, 1, 5, (first[w], 9), (first[w], 7))
            send2(w, layer, 5, 1, LAST, 1, 1)
            add(w, layer, 0, 7, (first[w], 4), (first[w], 10))
            send2(w, layer, 7, 0, LAST, 2, -1)

        over_layers(f)
        over_layers(g)

    def fwd2(w):
        def f(layer):
            wait(w, layer, FAR2)
            add(w, layer, 0, 5, (first[w], 9), (first[w], 7), (second[w], 0))
            send2(w, layer, 5, 0, LAST, 1, 1)
            add(w, layer, 1, 7, (first[w], 4), (first[w], 10), (second[w], 0))
            send2(w, layer, 7, 1, LAST, 2, -1)

        over_layers(f)

    def load_moments(w, layer):
        p, q = place(layer)
        slot = layer if w < 2 else 0
        pltpu.make_async_copy(ms[w].at[layer], wide[w].at[slot, 0], moment_sem.at[w, 0]).start()
        pltpu.make_async_copy(vs[w].at[layer], wide[w].at[slot, 1], moment_sem.at[w, 0]).start()
        pltpu.make_async_copy(weights[w].at[layer, rows(w, layer, p, q)], narrow[w].at[slot], moment_sem.at[w, 1]).start()

    def take_moments(w):
        take(wide[w], moment_sem.at[w, 0])
        take(narrow[w], moment_sem.at[w, 1])

    def step(w):
        if w < 2:
            take_moments(w)

        def f(layer):
            slot = layer if w < 2 else 0
            if w == 2:
                load_moments(w, layer)
            wait(w, layer, LAST)
            if w == 2:
                take_moments(w)

            def one(at, c):
                total = own[w][layer, 4, at, c].astype(jnp.float32)
                for ref, other in ((first[w], 5), (first[w], 11), (second[w], 1), (second[w], 2)):
                    total += ref[layer, other, at, c].astype(jnp.float32)
                g = total.astype(jnp.bfloat16)
                own[w][layer, 4, at, c] = g
                old = narrow[w][slot, at, c].astype(jnp.float32)
                second[w][layer, 1, at, c] = adamw(old, wide[w][slot, 0, at, c], wide[w][slot, 1, at, c], g.astype(jnp.float32))[0]

            blockwise(w, 2, one)
            for group, half, by in ((PARTS, 1, 1), (PARTS, 0, -1), (PARTS + 1, 0, 1), (PARTS + 1, 1, -1)):
                source = second[w].at[layer, 1, part(w, half)]
                send(w, layer, 2, group, source, home_there(w, layer, 0, by, half), to(layer, 1, by))
            pltpu.make_async_copy(own[w].at[layer, 4], gs[w].at[layer], store_sem.at[w, 0]).start()
            pltpu.make_async_copy(second[w].at[layer, 1], home(w, layer, 0), store_sem.at[w, 1]).start()

        over_layers(f, unroll=w == 2)

    def gather2(w):
        def f(layer):
            wait(w, layer, PARTS)
            for half, by in ((1, 1), (0, -1)):
                send(w, layer, 2, PARTS + 2, home(w, layer, -by, half), home_there(w, layer, -by, by, half), to(layer, 1, by))

        over_layers(f, unroll=w == 2)

    def give(w, layer, d, source=None):
        source = home(w, layer, d) if source is None else source
        for by in (1, -1):
            on = (by == 1) == (d % 2 == 0)
            if w < 2:
                send(w, layer, 3, ON + d // 2 if on else REST, source, home(w, layer, d), to(layer, 0, by))
            elif on:
                send(w, layer, 3, REST, source, staged[2 * layer + d % 2].at[2 + d // 2], to(layer, 0, by))

    def gather1(w):
        def f(layer):
            give(w, layer, 0, second[w].at[layer, 1])
            wait(w, layer, PARTS + 1)
            give(w, layer, 1)
            give(w, layer, 3)

        over_layers(f, unroll=w == 2)

    def gather1_far(w):
        def f(layer):
            wait(w, layer, PARTS + 2)
            give(w, layer, 2)

        over_layers(f, unroll=w == 2)

    def gather1_on(w):
        def f(layer, i):
            p, q = place(layer)
            wait(w, layer, ON + i, 2)
            for d, by in ((2 * i, 1), (1 + 2 * i, -1)):
                at = outs[w].at[layer, rows(w, layer, p - by, q + d)]
                send(w, layer, 3, REST, at, at, to(layer, 0, by))

        over_layers(f, 2)

    def finish(w):
        for layer in range(2):
            wait(w, layer, REST, 4 if w == 2 else 8)
        for leg, ref in enumerate((first[w], second[w], second[w], own[w].at[0] if w == 2 else first[w])):
            take(ref, send_sem.at[w, leg])
        for n in range(2):
            take(gs[w], store_sem.at[w, n])

    raw1(0)
    loads(0)
    over_layers(lambda layer: load_moments(0, layer))
    loads(1)
    fwd1(0)
    raw1(1)
    loads(2)
    raw2(0)
    fwd1(1)
    raw1(2)
    fwd2(0)
    raw2(1)
    fwd1(2)
    step(0)
    over_layers(lambda layer: load_moments(1, layer))
    fwd2(1)
    raw2(2)
    gather2(0)
    gather1(0)
    step(1)
    fwd2(2)
    gather1_far(0)
    gather2(1)
    gather1(1)
    step(2)
    gather1_on(0)
    gather1_far(1)
    gather2(2)
    gather1(2)
    gather1_on(1)
    gather1_far(2)
    for w in range(3):
        finish(w)


def spots(side, size, shift):
    me = lax.axis_index("dp")
    for layer in range(2):
        for way in range(2):
            for slot in range(side):
                far = (2 * way - 1) * (shift + slot // 2)
                d = (1 - way + slot // 2) % 2 + 2 * (slot % 2)
                a, b = (far, d) if layer == 0 else (d, far)
                block = (me // side + a + side) % side * side + (me % side + b + side) % side
                yield layer, way, slot, pl.ds(pl.multiple_of(block * size, ROWS), size)


def settle(side, *refs):
    gs, ms, vs, outs, staged = refs[:3], refs[3:6], refs[6:9], refs[9:11], refs[11:15]
    new_ms, new_vs, wholes = refs[15:18], refs[18:21], refs[21:24]
    g_at, m_at, v_at, w_at = refs[24:27], refs[27:30], refs[30:33], refs[33:36]
    moment_sem, store_sem, *copy_sem = refs[36:41]

    copies = []
    for w in range(2):
        pieces, size = w_at[w].shape[1:3]
        for layer in range(2):
            for n in range(pieces):
                at = pl.ds(n * size, size)
                copies.append((outs[w].at[layer, at], w_at[w].at[layer, n], wholes[w].at[layer, at], copy_sem[w].at[layer, n]))
    for layer, way, slot, at in spots(side, w_at[2].shape[2], 0):
        n = way * side + slot
        copies.append((staged[2 * layer + way].at[slot], w_at[2].at[layer, n], wholes[2].at[layer, at], copy_sem[2].at[layer, n]))

    for w in range(3):
        for n, (source, target) in enumerate(((gs, g_at), (ms, m_at), (vs, v_at))):
            pltpu.make_async_copy(source[w], target[w], moment_sem.at[w, n]).start()
    for source, buffer, _, sem in copies:
        pltpu.make_async_copy(source, buffer, sem).start()
    stores = []
    for w in range(3):
        for n, (source, target) in enumerate(((gs, g_at), (ms, m_at), (vs, v_at))):
            pltpu.make_async_copy(source[w], target[w], moment_sem.at[w, n]).wait()

        def body(r, _, w=w):
            for layer in range(2):
                at = pl.ds(pl.multiple_of(r * ROWS, ROWS), ROWS)
                for c in range(0, m_at[w].shape[2], COLS):
                    here = (layer, at, pl.ds(c, COLS))
                    _, m_at[w][here], v_at[w][here] = adamw(0.0, m_at[w][here], v_at[w][here], g_at[w][here].astype(jnp.float32))
            return 0

        lax.fori_loop(0, m_at[w].shape[1] // ROWS, body, 0)
        stores += [pltpu.make_async_copy(a[w], b[w], store_sem.at[w, n]) for n, (a, b) in enumerate(((m_at, new_ms), (v_at, new_vs)))]
        stores[-2].start()
        stores[-1].start()
    for source, buffer, target, sem in copies:
        pltpu.make_async_copy(source, buffer, sem).wait()
        stores.append(pltpu.make_async_copy(buffer, target, sem))
        stores[-1].start()
    for copy in stores:
        copy.wait()


def patch(side, layer, *refs):
    brought, whole, sem = refs[1:3], refs[3], refs[4]
    moves = []
    for here, way, slot, at in spots(side, brought[0].shape[1], 1):
        if here == layer:
            moves.append(pltpu.make_async_copy(brought[way].at[slot], whole.at[layer, at], sem.at[way, slot]))
            moves[-1].start()
    for move in moves:
        move.wait()


def solution(mesh):
    side = math.isqrt(mesh.shape["dp"])

    def on(ring, by):
        return [(x * side + y, (x + by) % side * side + y if ring == 0 else x * side + (y + by) % side) for x in range(side) for y in range(side)]

    def step(*arrays):
        weights, m, v = (arrays[i : i + 3] for i in (3, 6, 9))
        blocks = [one.shape[1:] for one in m]
        layers = m[0].shape[0]
        bf16, f32, dma = jnp.bfloat16, jnp.float32, pltpu.SemaphoreType.DMA
        anywhere = pl.BlockSpec(memory_space=pl.ANY)

        def call(f, name, inputs, outputs, scratch, params, held=0, limit=LIMIT, **more):
            return pl.pallas_call(
                f,
                out_shape=[jax.ShapeDtypeStruct(one.shape, one.dtype) for one in outputs],
                in_specs=[anywhere] * (len(inputs) - held) + [pl.BlockSpec(memory_space=pltpu.VMEM)] * held,
                out_specs=[anywhere] * len(outputs),
                scratch_shapes=scratch,
                compiler_params=pltpu.CompilerParams(vmem_limit_bytes=limit, **params),
                name=name,
                **more,
            )(*inputs)

        scratch = [pltpu.VMEM((layers, count, *b), bf16) for count in (8, 12, 3) for b in blocks]
        scratch += [pltpu.VMEM((k, 2, *blocks[w]), f32) for w, k in ((0, layers), (2, 1))]
        scratch += [pltpu.VMEM((k, *blocks[w]), bf16) for w, k in ((0, layers), (2, 1))]
        scratch += [dma((layers, len(BLOCKS)))] * 3 + [dma((3, 4)), dma((3,)), dma((3, 2)), dma((3, 2))]

        def exchange(*refs):
            head, (wide, wide2, narrow, narrow2), sems = refs[:30], refs[30:34], refs[34:]
            kernel(side, *head, wide, wide, wide2, narrow, narrow, narrow2, *sems)

        stage = jax.ShapeDtypeStruct((side, *blocks[2]), bf16)
        g = [jax.ShapeDtypeStruct(one.shape, bf16) for one in m]
        result = call(exchange, "exchange", arrays, [*weights[:2], *[stage] * 4, *g], scratch, {"collective_id": 0, "has_side_effects": True})
        whole, staged, g = result[:2], result[2:6], result[6:]
        brought = [lax.ppermute(one, "dp", on(n // 2, 1 - n % 2 * 2)) for n, one in enumerate(staged)]

        copied = [(layers, side, w.shape[1] // side, w.shape[2]) for w in weights[:2]] + [(layers, 2 * side, *blocks[2])]
        scratch = [pltpu.VMEM(one.shape, t) for t in (bf16, f32, f32) for one in m] + [pltpu.VMEM(shape, bf16) for shape in copied]
        scratch += [dma((3, 3)), dma((3, 2))] + [dma(shape[:2]) for shape in copied]
        cost = pl.CostEstimate(flops=18 * m[0].size, bytes_accessed=5 * weights[0].size, transcendentals=0)
        result = call(functools.partial(settle, side), "settle", [*g, *m, *v, *whole, *staged], [*m, *v, *weights], scratch, {}, limit=LIMIT * 8 // 9, cost_estimate=cost)
        *moments, gate, up, down = result
        few = {"held": 2, "limit": LIMIT // 8, "input_output_aliases": {0: 0}}
        for layer in range(layers):
            inputs = [down, *brought[2 * layer : 2 * layer + 2]]
            (down,) = call(functools.partial(patch, side, layer), "patch", inputs, [down], [dma((2, side))], {}, **few)
        return (gate, up, down, *moments)

    all_of, cut = P(None, None, None), P(None, "dp", None)
    return jax.shard_map(
        step,
        mesh=mesh,
        in_specs=(P(("rep", "dp"), None, None, None),) * 3 + (all_of,) * 3 + (cut,) * 6,
        out_specs=(P("rep", None, None),) * 3 + (P("rep", "dp", None),) * 6,
        check_vma=False,
    )
```

```python
import functools
import math

import jax
import jax.numpy as jnp
from jax import lax
from jax.experimental import pallas as pl
from jax.experimental.pallas import tpu as pltpu
from jax.sharding import PartitionSpec as P


MESH = pl.DeviceIdType.MESH
ROWS, COLS = 16, 256
LIMIT = 67043328
FAR, NEAR, FAR2, LAST, PARTS, ON, REST = 0, 2, 4, 5, 6, 9, 11
BLOCKS = (2, 2, 2, 4, 1, 4, 1, 1, 1, 2, 2, 8)


def adamw(w, m, v, g):
    m = 0.9 * m + 0.1 * g
    v = 0.95 * v + 0.05 * g * g
    step = m * lax.rsqrt(v + 1e-8) + 0.1 * w
    return (w - 0.02 * step).astype(jnp.bfloat16), m, v


def kernel(side, *refs):
    terms, weights, ms, vs = (refs[i : i + 3] for i in range(0, 12, 3))
    outs, staged, gs = refs[12:14], refs[14:18], refs[18:21]
    own, first, second, wide, narrow = (refs[i : i + 3] for i in range(21, 36, 3))
    recv_sem, send_sem, load_sem, moment_sem, store_sem = refs[36:41]

    me = lax.axis_index("dp")
    x, y = me // side, me % side
    for neighbour in ((x + 1) % side * side + y, (x + side - 1) % side * side + y, x * side + (y + 1) % side, x * side + (y + side - 1) % side):
        pl.semaphore_signal(pltpu.get_barrier_semaphore(), inc=1, device_id={"dp": neighbour}, device_id_type=MESH)
    pl.semaphore_wait(pltpu.get_barrier_semaphore(), 4)

    def place(layer):
        return x * (1 - layer) + y * layer, x * layer + y * (1 - layer)

    def index(layer, p, q):
        return (p + 2 * side) % side * (side * (1 - layer) + layer) + (q + 2 * side) % side * (1 - layer + side * layer)

    def to(layer, ring, by):
        p, q = place(layer)
        return {"dp": index(layer, p + by, q) if ring == 0 else index(layer, p, q + by)}

    def part(w, half):
        size = own[w].shape[2]
        cut = (size // ROWS + 1) // 2 * ROWS
        return (pl.ds(0, cut), pl.ds(cut, size - cut), pl.ds(0, size))[half]

    def rows(w, layer, p, q, half=2):
        inside = part(w, half)
        return pl.ds(pl.multiple_of(index(layer, p, q) * own[w].shape[2] + inside.start, ROWS), inside.size)

    def send(w, leg, group, source, target, device):
        pltpu.make_async_remote_copy(source, target, send_sem.at[w, leg], recv_sem.at[w, group], device_id=device, device_id_type=MESH).start()

    def take(ref, sem):
        pltpu.make_async_copy(ref, ref, sem).wait()

    def wait(w, group, blocks=None):
        take(own[w].at[:, pl.ds(0, blocks or BLOCKS[group])], recv_sem.at[w, group])

    def home(w, layer, d, half=2):
        p, q = place(layer)
        return staged[2 * layer + 1 - d % 2].at[d % side // 2, part(w, half)] if w == 2 else outs[w].at[layer, rows(w, layer, p, q + d, half)]

    def home_there(w, layer, d, by, half=2):
        return home(w, layer, (d - by) % side if w == 2 else d, half)

    def over_layers(f, times=1, unroll=False):
        if unroll:
            for n in range(2):
                f(n)
            return

        def body(n, _):
            f(n % 2, n // 2) if times > 1 else f(n)
            return 0

        lax.fori_loop(0, 2 * times, body, 0)

    def blockwise(w, half, f):
        inside = part(w, half)

        def body(r, _):
            at = pl.ds(pl.multiple_of(inside.start + r * ROWS, ROWS), ROWS)
            for c in range(0, own[w].shape[3], COLS):
                f(at, pl.ds(c, COLS))
            return 0

        lax.fori_loop(0, inside.size // ROWS, body, 0)

    def add(w, layer, half, slot, *others):
        def one(at, c):
            total = own[w][layer, slot, at, c].astype(jnp.float32)
            for ref, other in others:
                total += ref[layer, other, at, c].astype(jnp.float32)
            own[w][layer, slot, at, c] = total.astype(jnp.bfloat16)

        blockwise(w, half, one)


    def loads(w):
        def f(layer):
            p, q = place(layer)
            for slot, (far, d) in enumerate(((1, 2), (1, 1), (-1, 3), (-1, 0), (0, 0), (0, 1), (0, 2), (0, 3))):
                pltpu.make_async_copy(terms[w].at[0, layer, rows(w, layer, p + far, q + d)], own[w].at[layer, slot], load_sem.at[w]).start()

        over_layers(f)

    def raw1(w):
        def f(layer, i):
            p, q = place(layer)
            for k, d, by in ((0, 2 - i, 1), (2, 3 - 3 * i, -1)):
                source = terms[w].at[0, layer, rows(w, layer, p + 2, q + d)]
                send(w, 0, FAR + i, source, first[w].at[layer, k + i], to(layer, 0, by))

        def g(layer, i):
            p, q = place(layer)
            for k, d, by, group in ((4, 3 - 3 * i, 1, NEAR + 1 + 2 * i), (6, 2 - i, -1, NEAR + i)):
                source = terms[w].at[0, layer, rows(w, layer, p + by, q + d)]
                send(w, 0, group, source, first[w].at[layer, k + i], to(layer, 0, by))

        over_layers(f, 2)
        over_layers(g, 2)

    def fwd1(w):
        take(own[w], load_sem.at[w])
        for i in range(2):
            wait(w, FAR + i)

            def f(layer, i=i):
                for k, by, group in ((0, 1, NEAR + i), (2, -1, NEAR + 1 + 2 * i)):
                    add(w, layer, 2, k + i, (first[w], k + i))
                    send(w, 0, group, own[w].at[layer, k + i], first[w].at[layer, 8 + k + i], to(layer, 0, by))

            over_layers(f)

    def send2(w, layer, slot, half, group, target, by):
        at = part(w, half)
        send(w, 1, group, own[w].at[layer, slot, at], second[w].at[layer, target, at], to(layer, 1, by))

    def raw2(w):
        def f(layer):
            add(w, layer, 2, 6, (first[w], 8), (first[w], 6))
            send2(w, layer, 6, 0, FAR2, 0, 1)
            send2(w, layer, 6, 1, FAR2, 0, -1)

        def g(layer):
            add(w, layer, 1, 5, (first[w], 9), (first[w], 7))
            send2(w, layer, 5, 1, LAST, 1, 1)
            add(w, layer, 0, 7, (first[w], 4), (first[w], 10))
            send2(w, layer, 7, 0, LAST, 2, -1)

        wait(w, NEAR)
        over_layers(f)
        wait(w, NEAR + 1)
        over_layers(g)

    def fwd2(w):
        def f(layer):
            add(w, layer, 0, 5, (first[w], 9), (first[w], 7), (second[w], 0))
            send2(w, layer, 5, 0, LAST, 1, 1)
            add(w, layer, 1, 7, (first[w], 4), (first[w], 10), (second[w], 0))
            send2(w, layer, 7, 1, LAST, 2, -1)

        wait(w, FAR2)
        over_layers(f)

    def load_moments(w, layer):
        p, q = place(layer)
        slot = layer if w < 2 else 0
        pltpu.make_async_copy(ms[w].at[layer], wide[w].at[slot, 0], moment_sem.at[w, 0]).start()
        pltpu.make_async_copy(vs[w].at[layer], wide[w].at[slot, 1], moment_sem.at[w, 0]).start()
        pltpu.make_async_copy(weights[w].at[layer, rows(w, layer, p, q)], narrow[w].at[slot], moment_sem.at[w, 1]).start()

    def take_moments(w):
        take(wide[w], moment_sem.at[w, 0])
        take(narrow[w], moment_sem.at[w, 1])

    def step(w):
        wait(w, LAST)
        if w < 2:
            take_moments(w)

        def f(layer):
            slot = layer if w < 2 else 0
            if w == 2:
                load_moments(w, layer)
            if w == 2:
                take_moments(w)

            def one(at, c):
                total = own[w][layer, 4, at, c].astype(jnp.float32)
                for ref, other in ((first[w], 5), (first[w], 11), (second[w], 1), (second[w], 2)):
                    total += ref[layer, other, at, c].astype(jnp.float32)
                g = total.astype(jnp.bfloat16)
                own[w][layer, 4, at, c] = g
                old = narrow[w][slot, at, c].astype(jnp.float32)
                second[w][layer, 1, at, c] = adamw(old, wide[w][slot, 0, at, c], wide[w][slot, 1, at, c], g.astype(jnp.float32))[0]

            blockwise(w, 2, one)
            for group, half, by in ((PARTS, 1, 1), (PARTS, 0, -1), (PARTS + 1, 0, 1), (PARTS + 1, 1, -1)):
                source = second[w].at[layer, 1, part(w, half)]
                send(w, 2, group, source, home_there(w, layer, 0, by, half), to(layer, 1, by))
            pltpu.make_async_copy(own[w].at[layer, 4], gs[w].at[layer], store_sem.at[w]).start()
            pltpu.make_async_copy(second[w].at[layer, 1], home(w, layer, 0), store_sem.at[w]).start()

        over_layers(f, unroll=w == 2)

    def gather2(w):
        def f(layer):
            for half, by in ((1, 1), (0, -1)):
                send(w, 2, PARTS + 2, home(w, layer, -by, half), home_there(w, layer, -by, by, half), to(layer, 1, by))

        wait(w, PARTS)
        over_layers(f, unroll=w == 2)

    def give(w, layer, d, source=None):
        source = home(w, layer, d) if source is None else source
        for by in (1, -1):
            on = (by == 1) == (d % 2 == 0)
            if w < 2:
                send(w, 3, ON + d // 2 if on else REST, source, home(w, layer, d), to(layer, 0, by))
            elif on:
                send(w, 3, REST, source, staged[2 * layer + d % 2].at[2 + d // 2], to(layer, 0, by))

    def gather1(w):
        def f(layer):
            give(w, layer, 1)
            give(w, layer, 3)

        over_layers(lambda layer: give(w, layer, 0, second[w].at[layer, 1]), unroll=w == 2)
        wait(w, PARTS + 1)
        over_layers(f, unroll=w == 2)

    def gather1_far(w):
        wait(w, PARTS + 2)
        over_layers(lambda layer: give(w, layer, 2), unroll=w == 2)

    def gather1_on(w):
        for i in range(2):

            def f(layer, i=i):
                p, q = place(layer)
                for d, by in ((2 * i, 1), (1 + 2 * i, -1)):
                    at = outs[w].at[layer, rows(w, layer, p - by, q + d)]
                    send(w, 3, REST, at, at, to(layer, 0, by))

            wait(w, ON + i)
            over_layers(f)

    def finish(w):
        wait(w, REST, 4 if w == 2 else 8)
        for leg, ref in enumerate((first[w], second[w], second[w], own[w].at[0] if w == 2 else first[w])):
            take(ref, send_sem.at[w, leg])
        take(first[w].at[:, pl.ds(0, 2)], store_sem.at[w])

    raw1(0)
    loads(0)
    over_layers(lambda layer: load_moments(0, layer))
    loads(1)
    fwd1(0)
    raw1(1)
    loads(2)
    raw2(0)
    fwd1(1)
    raw1(2)
    fwd2(0)
    raw2(1)
    fwd1(2)
    step(0)
    over_layers(lambda layer: load_moments(1, layer))
    fwd2(1)
    raw2(2)
    gather2(0)
    gather1(0)
    step(1)
    fwd2(2)
    gather1_far(0)
    gather2(1)
    gather1(1)
    step(2)
    gather1_on(0)
    gather1_far(1)
    gather2(2)
    gather1(2)
    gather1_on(1)
    gather1_far(2)
    for w in range(3):
        finish(w)


def spots(side, size, shift):
    me = lax.axis_index("dp")
    for layer in range(2):
        for way in range(2):
            for slot in range(side):
                far = (2 * way - 1) * (shift + slot // 2)
                d = (1 - way + slot // 2) % 2 + 2 * (slot % 2)
                a, b = (far, d) if layer == 0 else (d, far)
                block = (me // side + a + side) % side * side + (me % side + b + side) % side
                yield layer, way, slot, pl.ds(pl.multiple_of(block * size, ROWS), size)


def settle(side, *refs):
    gs, ms, vs, outs, staged = refs[:3], refs[3:6], refs[6:9], refs[9:11], refs[11:15]
    new_ms, new_vs, wholes = refs[15:18], refs[18:21], refs[21:24]
    g_at, m_at, v_at, w_at = refs[24:27], refs[27:30], refs[30:33], refs[33:36]
    moment_sem, store_sem, *copy_sem = refs[36:41]

    copies = []
    for w in range(2):
        pieces, size = w_at[w].shape[1:3]
        for layer in range(2):
            for n in range(pieces):
                at = pl.ds(n * size, size)
                copies.append((outs[w].at[layer, at], w_at[w].at[layer, n], wholes[w].at[layer, at], copy_sem[w].at[layer, n]))
    for layer, way, slot, at in spots(side, w_at[2].shape[2], 0):
        n = way * side + slot
        copies.append((staged[2 * layer + way].at[slot], w_at[2].at[layer, n], wholes[2].at[layer, at], copy_sem[2].at[layer, n]))

    for w in range(3):
        for n, (source, target) in enumerate(((gs, g_at), (ms, m_at), (vs, v_at))):
            pltpu.make_async_copy(source[w], target[w], moment_sem.at[w, n]).start()
    for source, buffer, _, sem in copies:
        pltpu.make_async_copy(source, buffer, sem).start()
    stores = []
    for w in range(3):
        for n, (source, target) in enumerate(((gs, g_at), (ms, m_at), (vs, v_at))):
            pltpu.make_async_copy(source[w], target[w], moment_sem.at[w, n]).wait()

        def body(r, _, w=w):
            for layer in range(2):
                at = pl.ds(pl.multiple_of(r * ROWS, ROWS), ROWS)
                for c in range(0, m_at[w].shape[2], COLS):
                    here = (layer, at, pl.ds(c, COLS))
                    _, m_at[w][here], v_at[w][here] = adamw(0.0, m_at[w][here], v_at[w][here], g_at[w][here].astype(jnp.float32))
            return 0

        lax.fori_loop(0, m_at[w].shape[1] // ROWS, body, 0)
        stores += [pltpu.make_async_copy(a[w], b[w], store_sem.at[w, n]) for n, (a, b) in enumerate(((m_at, new_ms), (v_at, new_vs)))]
        stores[-2].start()
        stores[-1].start()
    for source, buffer, target, sem in copies:
        pltpu.make_async_copy(source, buffer, sem).wait()
        stores.append(pltpu.make_async_copy(buffer, target, sem))
        stores[-1].start()
    for copy in stores:
        copy.wait()


def patch(side, layer, *refs):
    brought, whole, sem = refs[1:3], refs[3], refs[4]
    moves = []
    for here, way, slot, at in spots(side, brought[0].shape[1], 1):
        if here == layer:
            moves.append(pltpu.make_async_copy(brought[way].at[slot], whole.at[layer, at], sem.at[way, slot]))
            moves[-1].start()
    for move in moves:
        move.wait()


def solution(mesh):
    side = math.isqrt(mesh.shape["dp"])

    def on(ring, by):
        return [(x * side + y, (x + by) % side * side + y if ring == 0 else x * side + (y + by) % side) for x in range(side) for y in range(side)]

    def step(*arrays):
        weights, m, v = (arrays[i : i + 3] for i in (3, 6, 9))
        blocks = [one.shape[1:] for one in m]
        layers = m[0].shape[0]
        bf16, f32, dma = jnp.bfloat16, jnp.float32, pltpu.SemaphoreType.DMA
        anywhere = pl.BlockSpec(memory_space=pl.ANY)

        def call(f, inputs, outputs, scratch, params, held=0, limit=LIMIT, **more):
            return pl.pallas_call(
                f,
                out_shape=[jax.ShapeDtypeStruct(one.shape, one.dtype) for one in outputs],
                in_specs=[anywhere] * (len(inputs) - held) + [pl.BlockSpec(memory_space=pltpu.VMEM)] * held,
                out_specs=[anywhere] * len(outputs),
                scratch_shapes=scratch,
                compiler_params=pltpu.CompilerParams(vmem_limit_bytes=limit, **params),
                **more,
            )(*inputs)

        scratch = [pltpu.VMEM((layers, count, *b), bf16) for count in (8, 12, 3) for b in blocks]
        scratch += [pltpu.VMEM((k, 2, *blocks[w]), f32) for w, k in ((0, layers), (2, 1))]
        scratch += [pltpu.VMEM((k, *blocks[w]), bf16) for w, k in ((0, layers), (2, 1))]
        scratch += [dma((3, len(BLOCKS))), dma((3, 4)), dma((3,)), dma((3, 2)), dma((3,))]

        def exchange(*refs):
            head, (wide, wide2, narrow, narrow2), sems = refs[:30], refs[30:34], refs[34:]
            kernel(side, *head, wide, wide, wide2, narrow, narrow, narrow2, *sems)

        stage = jax.ShapeDtypeStruct((side, *blocks[2]), bf16)
        g = [jax.ShapeDtypeStruct(one.shape, bf16) for one in m]
        result = call(exchange, arrays, [*weights[:2], *[stage] * 4, *g], scratch, {"collective_id": 0, "has_side_effects": True})
        whole, staged, g = result[:2], result[2:6], result[6:]
        brought = []
        for n, one in enumerate(staged):
            brought.append(lax.ppermute(one, "dp", on(n // 2, 1 - n % 2 * 2)))

        copied = [(layers, side, w.shape[1] // side, w.shape[2]) for w in weights[:2]] + [(layers, 2 * side, *blocks[2])]
        scratch = [pltpu.VMEM(one.shape, t) for t in (bf16, f32, f32) for one in m] + [pltpu.VMEM(shape, bf16) for shape in copied]
        scratch += [dma((3, 3)), dma((3, 2))] + [dma(shape[:2]) for shape in copied]
        cost = pl.CostEstimate(flops=18 * m[0].size, bytes_accessed=5 * weights[0].size, transcendentals=0)
        result = call(functools.partial(settle, side), [*g, *m, *v, *whole, *staged], [*m, *v, *weights], scratch, {}, limit=LIMIT * 8 // 9, cost_estimate=cost)
        *moments, gate, up, down = result
        few = {"held": 2, "limit": LIMIT // 8, "input_output_aliases": {0: 0}}
        for layer in range(layers):
            inputs = [down, *brought[2 * layer : 2 * layer + 2]]
            (down,) = call(functools.partial(patch, side, layer), inputs, [down], [dma((2, side))], {}, **few)
        return (gate, up, down, *moments)

    all_of, cut = P(None, None, None), P(None, "dp", None)
    return jax.shard_map(
        step,
        mesh=mesh,
        in_specs=(P(("rep", "dp"), None, None, None),) * 3 + (all_of,) * 3 + (cut,) * 6,
        out_specs=(P("rep", None, None),) * 3 + (P("rep", "dp", None),) * 6,
        check_vma=False,
    )
```

```python
import functools
import math

import jax
import jax.numpy as jnp
from jax import lax
from jax.experimental import pallas as pl
from jax.experimental.pallas import tpu as pltpu
from jax.sharding import PartitionSpec as P


MESH = pl.DeviceIdType.MESH
ROWS, COLS = 16, 256
LIMIT = 67043328
FAR, NEAR, FAR2, LAST, PARTS, ON, REST = 0, 2, 4, 5, 6, 9, 11
BLOCKS = (2, 2, 2, 4, 1, 4, 1, 1, 1, 2, 2, 8)


def adamw(w, m, v, g):
    m = 0.9 * m + 0.1 * g
    v = 0.95 * v + 0.05 * g * g
    step = m * lax.rsqrt(v + 1e-8) + 0.1 * w
    return (w - 0.02 * step).astype(jnp.bfloat16), m, v


def kernel(side, *refs):
    terms, weights, ms, vs = (refs[i : i + 3] for i in range(0, 12, 3))
    outs, staged, gs = refs[12:14], refs[14:18], refs[18:21]
    own, first, second, wide, narrow = (refs[i : i + 3] for i in range(21, 36, 3))
    recv_sem, send_sem, load_sem, moment_sem, store_sem = refs[36:41]

    me = lax.axis_index("dp")
    x, y = me // side, me % side
    for neighbour in ((x + 1) % side * side + y, (x + side - 1) % side * side + y, x * side + (y + 1) % side, x * side + (y + side - 1) % side):
        pl.semaphore_signal(pltpu.get_barrier_semaphore(), inc=1, device_id={"dp": neighbour}, device_id_type=MESH)
    pl.semaphore_wait(pltpu.get_barrier_semaphore(), 4)

    def place(layer):
        return x * (1 - layer) + y * layer, x * layer + y * (1 - layer)

    def index(layer, p, q):
        return (p + 2 * side) % side * (side * (1 - layer) + layer) + (q + 2 * side) % side * (1 - layer + side * layer)

    def to(layer, ring, by):
        p, q = place(layer)
        return {"dp": index(layer, p + by, q) if ring == 0 else index(layer, p, q + by)}

    def part(w, half):
        size = own[w].shape[2]
        cut = (size // ROWS + 1) // 2 * ROWS
        return (pl.ds(0, cut), pl.ds(cut, size - cut), pl.ds(0, size))[half]

    def rows(w, layer, p, q, half=2):
        inside = part(w, half)
        return pl.ds(pl.multiple_of(index(layer, p, q) * own[w].shape[2] + inside.start, ROWS), inside.size)

    def send(w, leg, group, source, target, device):
        pltpu.make_async_remote_copy(source, target, send_sem.at[w, leg], recv_sem.at[w, group], device_id=device, device_id_type=MESH).start()

    def take(ref, sem):
        pltpu.make_async_copy(ref, ref, sem).wait()

    def wait(w, group, blocks=None):
        take(own[w].at[:, pl.ds(0, blocks or BLOCKS[group])], recv_sem.at[w, group])

    def home(w, layer, d, half=2):
        p, q = place(layer)
        return staged[2 * layer + 1 - d % 2].at[d % side // 2, part(w, half)] if w == 2 else outs[w].at[layer, rows(w, layer, p, q + d, half)]

    def home_there(w, layer, d, by, half=2):
        return home(w, layer, (d - by) % side if w == 2 else d, half)

    def over_layers(f, times=1, unroll=False):
        if unroll:
            for n in range(2):
                f(n)
            return

        def body(n, _):
            f(n % 2, n // 2) if times > 1 else f(n)
            return 0

        lax.fori_loop(0, 2 * times, body, 0)

    def blockwise(w, half, f):
        inside = part(w, half)

        def body(r, _):
            at = pl.ds(pl.multiple_of(inside.start + r * ROWS, ROWS), ROWS)
            for c in range(0, own[w].shape[3], COLS):
                f(at, pl.ds(c, COLS))
            return 0

        lax.fori_loop(0, inside.size // ROWS, body, 0)

    def add(w, layer, half, slot, *others):
        def one(at, c):
            total = own[w][layer, slot, at, c].astype(jnp.float32)
            for ref, other in others:
                total += ref[layer, other, at, c].astype(jnp.float32)
            own[w][layer, slot, at, c] = total.astype(jnp.bfloat16)

        blockwise(w, half, one)


    def loads(w):
        def f(layer):
            p, q = place(layer)
            for slot, (far, d) in enumerate(((1, 2), (1, 1), (-1, 3), (-1, 0), (0, 0), (0, 1), (0, 2), (0, 3))):
                pltpu.make_async_copy(terms[w].at[0, layer, rows(w, layer, p + far, q + d)], own[w].at[layer, slot], load_sem.at[w]).start()

        over_layers(f)

    def raw1(w):
        def f(layer, i):
            p, q = place(layer)
            for k, d, by in ((0, 2 - i, 1), (2, 3 - 3 * i, -1)):
                source = terms[w].at[0, layer, rows(w, layer, p + 2, q + d)]
                send(w, 0, FAR + i, source, first[w].at[layer, k + i], to(layer, 0, by))

        def g(layer, i):
            p, q = place(layer)
            for k, d, by, group in ((4, 3 - 3 * i, 1, NEAR + 1 + 2 * i), (6, 2 - i, -1, NEAR + i)):
                source = terms[w].at[0, layer, rows(w, layer, p + by, q + d)]
                send(w, 0, group, source, first[w].at[layer, k + i], to(layer, 0, by))

        over_layers(f, 2)
        over_layers(g, 2)

    def fwd1(w):
        take(own[w], load_sem.at[w])
        for i in range(2):
            wait(w, FAR + i)

            def f(layer, i=i):
                for k in (0, 2):
                    add(w, layer, 2, k + i, (first[w], k + i))
                for k, by, group in ((0, 1, NEAR + i), (2, -1, NEAR + 1 + 2 * i)):
                    send(w, 0, group, own[w].at[layer, k + i], first[w].at[layer, 8 + k + i], to(layer, 0, by))

            over_layers(f)

    def send2(w, layer, slot, half, group, target, by):
        at = part(w, half)
        send(w, 1, group, own[w].at[layer, slot, at], second[w].at[layer, target, at], to(layer, 1, by))

    def raw2(w):
        def f(layer):
            add(w, layer, 2, 6, (first[w], 8), (first[w], 6))
            send2(w, layer, 6, 0, FAR2, 0, 1)
            send2(w, layer, 6, 1, FAR2, 0, -1)

        def g(layer):
            add(w, layer, 1, 5, (first[w], 9), (first[w], 7))
            add(w, layer, 0, 7, (first[w], 4), (first[w], 10))
            send2(w, layer, 5, 1, LAST, 1, 1)
            send2(w, layer, 7, 0, LAST, 2, -1)

        wait(w, NEAR)
        over_layers(f)
        wait(w, NEAR + 1)
        over_layers(g)

    def fwd2(w):
        def f(layer):
            add(w, layer, 0, 5, (first[w], 9), (first[w], 7), (second[w], 0))
            add(w, layer, 1, 7, (first[w], 4), (first[w], 10), (second[w], 0))
            send2(w, layer, 5, 0, LAST, 1, 1)
            send2(w, layer, 7, 1, LAST, 2, -1)

        wait(w, FAR2)
        over_layers(f)

    def load_moments(w, layer):
        p, q = place(layer)
        slot = layer if w < 2 else 0
        pltpu.make_async_copy(ms[w].at[layer], wide[w].at[slot, 0], moment_sem.at[w, 0]).start()
        pltpu.make_async_copy(vs[w].at[layer], wide[w].at[slot, 1], moment_sem.at[w, 0]).start()
        pltpu.make_async_copy(weights[w].at[layer, rows(w, layer, p, q)], narrow[w].at[slot], moment_sem.at[w, 1]).start()

    def take_moments(w):
        take(wide[w], moment_sem.at[w, 0])
        take(narrow[w], moment_sem.at[w, 1])

    def step(w):
        wait(w, LAST)
        if w < 2:
            take_moments(w)

        def f(layer):
            slot = layer if w < 2 else 0
            if w == 2:
                load_moments(w, layer)
            if w == 2:
                take_moments(w)

            def one(at, c):
                total = own[w][layer, 4, at, c].astype(jnp.float32)
                for ref, other in ((first[w], 5), (first[w], 11), (second[w], 1), (second[w], 2)):
                    total += ref[layer, other, at, c].astype(jnp.float32)
                g = total.astype(jnp.bfloat16)
                own[w][layer, 4, at, c] = g
                old = narrow[w][slot, at, c].astype(jnp.float32)
                second[w][layer, 1, at, c] = adamw(old, wide[w][slot, 0, at, c], wide[w][slot, 1, at, c], g.astype(jnp.float32))[0]

            blockwise(w, 2, one)
            for group, half, by in ((PARTS, 1, 1), (PARTS, 0, -1), (PARTS + 1, 0, 1), (PARTS + 1, 1, -1)):
                source = second[w].at[layer, 1, part(w, half)]
                send(w, 2, group, source, home_there(w, layer, 0, by, half), to(layer, 1, by))
            pltpu.make_async_copy(own[w].at[layer, 4], gs[w].at[layer], store_sem.at[w]).start()
            pltpu.make_async_copy(second[w].at[layer, 1], home(w, layer, 0), store_sem.at[w]).start()

        over_layers(f, unroll=w == 2)

    def gather2(w):
        def f(layer):
            for half, by in ((1, 1), (0, -1)):
                send(w, 2, PARTS + 2, home(w, layer, -by, half), home_there(w, layer, -by, by, half), to(layer, 1, by))

        wait(w, PARTS)
        over_layers(f, unroll=w == 2)

    def give(w, layer, d, source=None):
        source = home(w, layer, d) if source is None else source
        for by in (1, -1):
            on = (by == 1) == (d % 2 == 0)
            if w < 2:
                send(w, 3, ON + d // 2 if on else REST, source, home(w, layer, d), to(layer, 0, by))
            elif on:
                send(w, 3, REST, source, staged[2 * layer + d % 2].at[2 + d // 2], to(layer, 0, by))

    def gather1(w):
        def f(layer):
            give(w, layer, 1)
            give(w, layer, 3)

        over_layers(lambda layer: give(w, layer, 0, second[w].at[layer, 1]), unroll=w == 2)
        wait(w, PARTS + 1)
        over_layers(f, unroll=w == 2)

    def gather1_far(w):
        wait(w, PARTS + 2)
        over_layers(lambda layer: give(w, layer, 2), unroll=w == 2)

    def gather1_on(w):
        for i in range(2):

            def f(layer, i=i):
                p, q = place(layer)
                for d, by in ((2 * i, 1), (1 + 2 * i, -1)):
                    at = outs[w].at[layer, rows(w, layer, p - by, q + d)]
                    send(w, 3, REST, at, at, to(layer, 0, by))

            wait(w, ON + i)
            over_layers(f)

    def finish(w):
        wait(w, REST, 4 if w == 2 else 8)
        for leg, ref in enumerate((first[w], second[w], second[w], own[w].at[0] if w == 2 else first[w])):
            take(ref, send_sem.at[w, leg])
        take(first[w].at[:, pl.ds(0, 2)], store_sem.at[w])

    raw1(0)
    loads(0)
    over_layers(lambda layer: load_moments(0, layer))
    loads(1)
    fwd1(0)
    raw1(1)
    loads(2)
    raw2(0)
    fwd1(1)
    raw1(2)
    fwd2(0)
    raw2(1)
    fwd1(2)
    step(0)
    over_layers(lambda layer: load_moments(1, layer))
    fwd2(1)
    raw2(2)
    gather2(0)
    gather1(0)
    step(1)
    fwd2(2)
    gather1_far(0)
    gather2(1)
    gather1(1)
    step(2)
    gather1_on(0)
    gather1_far(1)
    gather2(2)
    gather1(2)
    gather1_on(1)
    gather1_far(2)
    finish(0)
    finish(1)
    finish(2)


def spots(side, size, shift):
    me = lax.axis_index("dp")
    for layer in range(2):
        for way in range(2):
            for slot in range(side):
                far = (2 * way - 1) * (shift + slot // 2)
                d = (1 - way + slot // 2) % 2 + 2 * (slot % 2)
                a, b = (far, d) if layer == 0 else (d, far)
                block = (me // side + a + side) % side * side + (me % side + b + side) % side
                yield layer, way, slot, pl.ds(pl.multiple_of(block * size, ROWS), size)


def settle(side, *refs):
    gs, ms, vs, outs, staged = refs[:3], refs[3:6], refs[6:9], refs[9:11], refs[11:15]
    new_ms, new_vs, wholes = refs[15:18], refs[18:21], refs[21:24]
    g_at, m_at, v_at, w_at = refs[24:27], refs[27:30], refs[30:33], refs[33:36]
    moment_sem, store_sem, *copy_sem = refs[36:41]

    copies = []
    for w in range(2):
        pieces, size = w_at[w].shape[1:3]
        for layer in range(2):
            for n in range(pieces):
                at = pl.ds(n * size, size)
                copies.append((outs[w].at[layer, at], w_at[w].at[layer, n], wholes[w].at[layer, at], copy_sem[w].at[layer, n]))
    for layer, way, slot, at in spots(side, w_at[2].shape[2], 0):
        n = way * side + slot
        copies.append((staged[2 * layer + way].at[slot], w_at[2].at[layer, n], wholes[2].at[layer, at], copy_sem[2].at[layer, n]))

    for w in range(3):
        for n, (source, target) in enumerate(((gs, g_at), (ms, m_at), (vs, v_at))):
            pltpu.make_async_copy(source[w], target[w], moment_sem.at[w, n]).start()
    for source, buffer, _, sem in copies:
        pltpu.make_async_copy(source, buffer, sem).start()
    stores = []
    for w in range(3):
        for n, (source, target) in enumerate(((gs, g_at), (ms, m_at), (vs, v_at))):
            pltpu.make_async_copy(source[w], target[w], moment_sem.at[w, n]).wait()

        def body(r, _, w=w):
            for layer in range(2):
                at = pl.ds(pl.multiple_of(r * ROWS, ROWS), ROWS)
                for c in range(0, m_at[w].shape[2], COLS):
                    here = (layer, at, pl.ds(c, COLS))
                    _, m_at[w][here], v_at[w][here] = adamw(0.0, m_at[w][here], v_at[w][here], g_at[w][here].astype(jnp.float32))
            return 0

        lax.fori_loop(0, m_at[w].shape[1] // ROWS, body, 0)
        stores += [pltpu.make_async_copy(a[w], b[w], store_sem.at[w, n]) for n, (a, b) in enumerate(((m_at, new_ms), (v_at, new_vs)))]
        stores[-2].start()
        stores[-1].start()
    for source, buffer, target, sem in copies:
        pltpu.make_async_copy(source, buffer, sem).wait()
        stores.append(pltpu.make_async_copy(buffer, target, sem))
        stores[-1].start()
    for copy in stores:
        copy.wait()


def patch(side, layer, *refs):
    brought, whole, sem = refs[1:3], refs[3], refs[4]
    moves = []
    for here, way, slot, at in spots(side, brought[0].shape[1], 1):
        if here == layer:
            moves.append(pltpu.make_async_copy(brought[way].at[slot], whole.at[layer, at], sem.at[way, slot]))
            moves[-1].start()
    for move in moves:
        move.wait()


def solution(mesh):
    side = math.isqrt(mesh.shape["dp"])

    def on(ring, by):
        return [(x * side + y, (x + by) % side * side + y if ring == 0 else x * side + (y + by) % side) for x in range(side) for y in range(side)]

    def step(*arrays):
        weights, m, v = (arrays[i : i + 3] for i in (3, 6, 9))
        blocks = [one.shape[1:] for one in m]
        layers = m[0].shape[0]
        bf16, f32, dma = jnp.bfloat16, jnp.float32, pltpu.SemaphoreType.DMA
        anywhere = pl.BlockSpec(memory_space=pl.ANY)

        def call(f, inputs, outputs, scratch, params, held=0, limit=LIMIT, **more):
            return pl.pallas_call(
                f,
                out_shape=[jax.ShapeDtypeStruct(one.shape, one.dtype) for one in outputs],
                in_specs=[anywhere] * (len(inputs) - held) + [pl.BlockSpec(memory_space=pltpu.VMEM)] * held,
                out_specs=[anywhere] * len(outputs),
                scratch_shapes=scratch,
                compiler_params=pltpu.CompilerParams(vmem_limit_bytes=limit, **params),
                **more,
            )(*inputs)

        scratch = [pltpu.VMEM((layers, count, *b), bf16) for count in (8, 12, 3) for b in blocks]
        scratch += [pltpu.VMEM((k, 2, *blocks[w]), f32) for w, k in ((0, layers), (2, 1))]
        scratch += [pltpu.VMEM((k, *blocks[w]), bf16) for w, k in ((0, layers), (2, 1))]
        scratch += [dma((3, len(BLOCKS))), dma((3, 4)), dma((3,)), dma((3, 2)), dma((3,))]

        def exchange(*refs):
            head, (wide, wide2, narrow, narrow2), sems = refs[:30], refs[30:34], refs[34:]
            kernel(side, *head, wide, wide, wide2, narrow, narrow, narrow2, *sems)

        stage = jax.ShapeDtypeStruct((side, *blocks[2]), bf16)
        g = [jax.ShapeDtypeStruct(one.shape, bf16) for one in m]
        result = call(exchange, arrays, [*weights[:2], *[stage] * 4, *g], scratch, {"collective_id": 0, "has_side_effects": True})
        whole, staged, g = result[:2], result[2:6], result[6:]
        brought = []
        for n, one in enumerate(staged):
            brought.append(lax.ppermute(one, "dp", on(n // 2, 1 - n % 2 * 2)))

        copied = [(layers, side, w.shape[1] // side, w.shape[2]) for w in weights[:2]] + [(layers, 2 * side, *blocks[2])]
        scratch = [pltpu.VMEM(one.shape, t) for t in (bf16, f32, f32) for one in m] + [pltpu.VMEM(shape, bf16) for shape in copied]
        scratch += [dma((3, 3)), dma((3, 2))] + [dma(shape[:2]) for shape in copied]
        cost = pl.CostEstimate(flops=18 * m[0].size, bytes_accessed=5 * weights[0].size, transcendentals=0)
        result = call(functools.partial(settle, side), [*g, *m, *v, *whole, *staged], [*m, *v, *weights], scratch, {}, limit=LIMIT * 8 // 9, cost_estimate=cost)
        *moments, gate, up, down = result
        few = {"held": 2, "limit": LIMIT // 8, "input_output_aliases": {0: 0}}
        for layer in range(layers):
            inputs = [down, *brought[2 * layer : 2 * layer + 2]]
            (down,) = call(functools.partial(patch, side, layer), inputs, [down], [dma((2, side))], {}, **few)
        return (gate, up, down, *moments)

    all_of, cut = P(None, None, None), P(None, "dp", None)
    return jax.shard_map(
        step,
        mesh=mesh,
        in_specs=(P(("rep", "dp"), None, None, None),) * 3 + (all_of,) * 3 + (cut,) * 6,
        out_specs=(P("rep", None, None),) * 3 + (P("rep", "dp", None),) * 6,
        check_vma=False,
    )
```
